32 devices in a mesh: rep: 4 (over y, core), ep: 4 (over z), tp: 2 (over x).
Axes of the slice: x: 2, y: 2, z: 4, core: 2. Of those that a mesh axis runs over, the one named last changes fastest.
Arguments:
- tokens: bfloat16 [128, 6144], P(('rep', 'ep'), 'tp'), may hold values from -6 to 6
- expert_ids: int32 [128, 2], P(('rep', 'ep')), may hold values from 0 to 3, as said below
- replicas: int32 [128, 2], P(('rep', 'ep')), may hold values from 0 to 3, as said below
- scores: float32 [128, 2], P(('rep', 'ep')), may hold values from -8 to 8
- w_gate: bfloat16 [4, 6144, 1024], P('ep', None, 'tp'), may hold values from -0.078125 to 0.078125
- w_up: bfloat16 [4, 6144, 1024], P('ep', None, 'tp'), may hold values from -0.078125 to 0.078125
- w_down: bfloat16 [4, 1024, 6144], P('ep', 'tp'), may hold values from -0.1875 to 0.1875
Outputs:
- moe_out: bfloat16 [128, 6144], P(('rep', 'ep'), 'tp')
- load_counts: int32 [4, 4], replicated
The draws below stay inside these ranges and needn't reach their ends.
Inputs may be any that keep to these rules, and one draw needn't show every extreme that they name: `expert_ids`: each row names 2 different experts. In the rows of one device one expert is named by every row. `replicas`: in the rows of one device at most 2 pairs name the same expert with the same replica pick, and some expert and pick reach 2.
All inputs are finite; a program needn't handle non-finite values.
Results may differ from the reference program's by a relative error of at most 0.008.
Values may be sent and summed in bfloat16 or wider, within the bound.
No kernel may reach another device: no remote copies, remote signals or barrier semaphores. Data moves between devices by JAX's collectives and lax.ppermute only.
A program may use at most 64 MiB of HBM per device.

```python
import jax
import jax.numpy as jnp
from jax import lax

D = 6144
FFE = 1024
TOK_DEV = 8
REPL = 4
EXPERTS = 4
TOPK = 2
TOKENS = 128
N_REP = 4
N_EP = 4


def routing_tables(key):
    blocks = TOKENS // TOK_DEV
    key_hot = jax.random.fold_in(key, 101)
    key_rest = jax.random.fold_in(key, 102)
    key_roll = jax.random.fold_in(key, 103)
    key_offset = jax.random.fold_in(key, 104)
    hot_block = jax.random.randint(key_hot, (blocks,), 0, EXPERTS).astype(jnp.int32)
    hot_token = jnp.repeat(hot_block, TOK_DEV)
    raw_bits = jax.random.randint(key_rest, (TOKENS, EXPERTS), 0, 1 << 20).astype(jnp.int32)
    column_ids = jnp.arange(EXPERTS, dtype=jnp.int32)
    ranked = raw_bits * EXPERTS + column_ids[None, :]
    ranked = jnp.where(column_ids[None, :] == hot_token[:, None], -1, ranked)
    unused, others = lax.top_k(ranked, TOPK - 1)
    chosen = jnp.concatenate([hot_token[:, None], others.astype(jnp.int32)], 1)
    rolled = jax.random.randint(key_roll, (TOKENS, 1), 0, TOPK).astype(jnp.int32)
    position = (jnp.arange(TOPK, dtype=jnp.int32)[None, :] + rolled) % TOPK
    chosen = jnp.take_along_axis(chosen, position, 1)
    named = jnp.sum((chosen[:, :, None] == column_ids[None, None, :]).astype(jnp.int32), 1)
    named_blocks = named.reshape(blocks, TOK_DEV, EXPERTS)
    earlier = (jnp.cumsum(named_blocks, 1) - named_blocks).reshape(TOKENS, EXPERTS)
    offsets = jax.random.randint(key_offset, (blocks, EXPERTS), 0, REPL).astype(jnp.int32)
    offset_token = jnp.repeat(offsets, TOK_DEV, axis=0)
    copy_table = (earlier + offset_token) % REPL
    copies = jnp.take_along_axis(copy_table, chosen, 1)
    return (chosen.astype(jnp.int32), copies.astype(jnp.int32))


def draw_expert_ids(key, part):
    chosen, copies = routing_tables(key)
    return chosen


def draw_replicas(key, part):
    chosen, copies = routing_tables(key)
    return copies


def block_scale(rng, extent, split, smallest, largest):
    loudness = 1.0
    for dim, parts in split:
        draws = jax.random.uniform(jax.random.fold_in(jax.random.fold_in(rng, 6), dim), (parts,), jnp.float32, smallest / len(split), largest / len(split))
        loudness = loudness * jnp.repeat(jnp.exp(draws), extent[dim] // parts).reshape((-1,) + (1,) * (len(extent) - 1 - dim))
    return loudness


def scatter_about(own_key, extent, deviation, most, shards=(), held_as=jnp.bfloat16):
    factor_of = block_scale(own_key, extent, shards, -0.22, 0.18) if shards else 1.0
    entries = jax.random.normal(own_key, extent, jnp.float32) * deviation * factor_of
    return jnp.minimum(jnp.maximum(entries, -most), most).astype(held_as)


def setup_inputs(seed: int = 0) -> dict:
    key_list = jax.random.split(jax.random.key(seed), 8)
    tokens = scatter_about(key_list[0], (TOKENS, D), 1.0, 6.0, ((0, 16), (1, 2)))
    expert_ids = draw_expert_ids(jax.random.fold_in(key_list[7], 71), 0)
    replicas = draw_replicas(jax.random.fold_in(key_list[7], 71), 0)
    scores = scatter_about(key_list[3], (TOKENS, TOPK), 2.0, 8.0, ((0, 16),), jnp.float32)
    w_gate = scatter_about(key_list[4], (EXPERTS, D, FFE), D ** -0.5, 0.078125, ((0, 4), (2, 2)))
    w_up = scatter_about(key_list[5], (EXPERTS, D, FFE), D ** -0.5, 0.078125, ((0, 4), (2, 2)))
    w_down = scatter_about(key_list[6], (EXPERTS, FFE, D), FFE ** -0.5, 0.1875, ((0, 4), (1, 2)))
    return {"tokens": tokens, "expert_ids": expert_ids, "replicas": replicas, "scores": scores, "w_gate": w_gate, "w_up": w_up, "w_down": w_down}


route_scale = 2.5


def reference(tokens, expert_ids, replicas, scores, w_gate, w_up, w_down):
    sigmoid_scores = jax.nn.sigmoid(scores)
    weights = sigmoid_scores / jnp.sum(sigmoid_scores, 1, keepdims=True) * route_scale

    def serve(running, expert):
        matched = expert_ids == expert
        coefficient = jnp.sum(jnp.where(matched, weights, jnp.zeros_like(weights)), 1)
        gate_pre = jnp.dot(tokens, w_gate[expert], preferred_element_type=jnp.float32)
        up_pre = jnp.dot(tokens, w_up[expert], preferred_element_type=jnp.float32)
        hidden = (jax.nn.silu(gate_pre) * up_pre).astype(jnp.bfloat16)
        expert_out = jnp.dot(hidden, w_down[expert], preferred_element_type=jnp.float32).astype(jnp.bfloat16)
        return running + coefficient[:, None] * expert_out.astype(jnp.float32), None

    start_total = jnp.zeros((TOKENS, D), jnp.float32)
    running, unused = lax.scan(serve, start_total, jnp.arange(EXPERTS, dtype=jnp.int32))
    moe_out = running.astype(jnp.bfloat16)
    source_group = (jnp.arange(TOKENS, dtype=jnp.int32) // (TOK_DEV * N_EP))[:, None]
    target = (source_group + replicas * (N_REP // REPL)) % N_REP
    group_hit = target.reshape(-1)[:, None, None] == jnp.arange(N_REP, dtype=jnp.int32)[None, :, None]
    expert_hit = expert_ids.reshape(-1)[:, None, None] == jnp.arange(EXPERTS, dtype=jnp.int32)[None, None, :]
    load_counts = jnp.sum((group_hit & expert_hit).astype(jnp.int32), 0)
    return moe_out, load_counts
```

```python
import functools

import jax
import jax.numpy as jnp
from jax import lax
from jax.experimental import pallas as pl
from jax.experimental.pallas import tpu as pltpu
from jax.sharding import PartitionSpec as P

REPL = 4
LANES = 128
SUBLANES = 8
MIB = 1 << 20

route_scale = 2.5


def shift(array, axis, count, step):
    return lax.ppermute(array, axis, [(i, (i + step) % count) for i in range(count)])


def fetch_kernel(pieces, gate_hbm, up_hbm, down_hbm, gate_vmem, up_vmem, down_vmem, sems):
    copies = []
    for source, target in ((gate_hbm, gate_vmem), (up_hbm, up_vmem), (down_hbm, down_vmem)):
        rows = source.shape[0] // pieces
        for piece in range(pieces):
            window = pl.ds(piece * rows, rows)
            copies.append(
                pltpu.make_async_copy(source.at[window], target.at[window], sems.at[len(copies)])
            )
    for copy in copies:
        copy.start()
    for copy in copies:
        copy.wait()


def fetch_weights(gate, up, down):
    pieces = 4
    size = 2 * (gate.size + up.size + down.size)
    return pl.pallas_call(
        functools.partial(fetch_kernel, pieces),
        out_shape=[pltpu.VMEM(w.shape, w.dtype) for w in (gate, up, down)],
        in_specs=[pl.BlockSpec(memory_space=pltpu.HBM)] * 3,
        out_specs=[pl.BlockSpec(memory_space=pltpu.VMEM)] * 3,
        scratch_shapes=[pltpu.SemaphoreType.DMA((3 * pieces,))],
        compiler_params=pltpu.CompilerParams(vmem_limit_bytes=32 * MIB),
        cost_estimate=pl.CostEstimate(flops=10**8, bytes_accessed=size, transcendentals=0),
        name="fetch_weights",
    )(gate, up, down)


def own_kernel(x_ref, gate_ref, up_ref, gate_out, up_out):
    part = x_ref.shape[1]
    base = pl.multiple_of(lax.axis_index("tp") * part, part)
    rows = pl.ds(base, part)
    x = x_ref[...]
    gate_out[...] = jnp.dot(x, gate_ref[rows, :], preferred_element_type=jnp.float32)
    up_out[...] = jnp.dot(x, up_ref[rows, :], preferred_element_type=jnp.float32)


def hidden_kernel(tp_count, *refs):
    others = refs[: tp_count - 1]
    gate_acc, up_acc, gate_ref, up_ref, down_ref = refs[tp_count - 1 : tp_count + 4]
    hidden_out = refs[tp_count + 4]
    partial_outs = refs[tp_count + 5 :]
    me = lax.axis_index("tp")
    gate = gate_acc[...]
    up = up_acc[...]
    for step, other in enumerate(others, 1):
        part = other.shape[1]
        sender = lax.rem(me - step + tp_count, tp_count)
        rows = pl.ds(pl.multiple_of(sender * part, part), part)
        x = other[...]
        gate += jnp.dot(x, gate_ref[rows, :], preferred_element_type=jnp.float32)
        up += jnp.dot(x, up_ref[rows, :], preferred_element_type=jnp.float32)
    hidden = (gate / (1.0 + jnp.exp(-gate)) * up).astype(jnp.bfloat16)
    hidden_out[...] = hidden
    for step, out in enumerate(partial_outs, 1):
        part = out.shape[1]
        target = lax.rem(me + step, tp_count)
        columns = pl.ds(pl.multiple_of(target * part, part), part)
        out[...] = jnp.dot(
            hidden, down_ref[:, columns], preferred_element_type=jnp.float32
        ).astype(jnp.bfloat16)


def down_kernel(hidden_ref, down_ref, out_ref):
    part = out_ref.shape[1]
    columns = pl.ds(pl.multiple_of(lax.axis_index("tp") * part, part), part)
    out_ref[...] = jnp.dot(
        hidden_ref[...], down_ref[:, columns], preferred_element_type=jnp.float32
    )


def vmem_call(kernel, name, outs, args, flops, grant=24):
    return pl.pallas_call(
        kernel,
        out_shape=outs,
        in_specs=[pl.BlockSpec(memory_space=pltpu.VMEM)] * len(args),
        out_specs=[pl.BlockSpec(memory_space=pltpu.VMEM)] * len(outs),
        compiler_params=pltpu.CompilerParams(vmem_limit_bytes=grant * MIB),
        cost_estimate=pl.CostEstimate(flops=flops, bytes_accessed=MIB, transcendentals=0),
        name=name,
    )(*args)


def per_device(tokens, expert_ids, replicas, scores, w_gate, w_up, w_down):
    rep_count = lax.axis_size("rep")
    ep_count = lax.axis_size("ep")
    tp_count = lax.axis_size("tp")
    tok_rows, part = tokens.shape
    features = part * tp_count
    ffe = w_gate.shape[2]
    rows = ep_count * tok_rows
    bf16, f32 = jnp.bfloat16, jnp.float32
    arr = jax.ShapeDtypeStruct

    blocks = [tokens] + [shift(tokens, "ep", ep_count, s) for s in range(1, ep_count)]
    gate_w, up_w, down_w = fetch_weights(w_gate[0], w_up[0], w_down[0])
    own = jnp.concatenate(blocks, 0)
    others = [shift(own, "tp", tp_count, s) for s in range(1, tp_count)]

    dot_flops = 2 * rows * part * ffe
    gate_acc, up_acc = vmem_call(
        own_kernel, "own_features", [arr((rows, ffe), f32)] * 2, (own, gate_w, up_w), 2 * dot_flops
    )
    hidden, *partials = vmem_call(
        functools.partial(hidden_kernel, tp_count),
        "hidden",
        [arr((rows, ffe), bf16)] + [arr((rows, part), bf16)] * (tp_count - 1),
        (*others, gate_acc, up_acc, gate_w, up_w, down_w),
        3 * (tp_count - 1) * dot_flops,
    )
    arrived = [shift(p, "tp", tp_count, s) for s, p in enumerate(partials, 1)]
    (mine,) = vmem_call(
        down_kernel, "own_down", [arr((rows, part), f32)], (hidden, down_w), dot_flops
    )
    for piece in arrived:
        mine = mine + piece.astype(f32)
    expert_out = mine.astype(bf16).reshape(ep_count, tok_rows, part)

    target = (lax.axis_index("rep") + replicas * (rep_count // REPL)) % rep_count
    cells = (target * ep_count + expert_ids).reshape(-1)
    cell_count = rep_count * ep_count
    counts = jnp.sum(
        (cells[:, None] == jnp.arange(cell_count, dtype=jnp.int32)[None, :]).astype(jnp.int32), 0
    )
    span = 1
    while span < rep_count:
        swap = [(i, i ^ span) for i in range(rep_count)]
        counts = counts + lax.ppermute(counts, "rep", swap)
        span *= 2
    width = -(-cell_count // (tok_rows * LANES)) * LANES
    carried = jnp.pad(counts, (0, tok_rows * width - cell_count)).astype(bf16)
    carried = carried.reshape(tok_rows, width)

    message = jnp.concatenate([expert_out[0], carried], 1)
    back = [message] + [
        shift(jnp.concatenate([expert_out[s], carried], 1), "ep", ep_count, -s)
        for s in range(1, ep_count)
    ]
    sigmoid_scores = jax.nn.sigmoid(scores)
    weights = sigmoid_scores / jnp.sum(sigmoid_scores, 1, keepdims=True) * route_scale
    me = lax.axis_index("ep")
    total = 0.0
    count_total = 0.0
    for s, piece in enumerate(back):
        expert = (me + s) % ep_count
        coefficient = jnp.sum(jnp.where(expert_ids == expert, weights, 0.0), 1, keepdims=True)
        total = total + coefficient * piece[:, :part].astype(f32)
        count_total = count_total + piece[:, part:].astype(f32)
    load_counts = count_total.reshape(-1)[:cell_count].astype(jnp.int32)
    return total.astype(bf16), load_counts.reshape(rep_count, ep_count)


def solution(mesh):
    placed = (
        P(("rep", "ep"), "tp"),
        P(("rep", "ep"), None),
        P(("rep", "ep"), None),
        P(("rep", "ep"), None),
        P("ep", None, "tp"),
        P("ep", None, "tp"),
        P("ep", "tp", None),
    )
    return jax.shard_map(
        per_device,
        mesh=mesh,
        in_specs=placed,
        out_specs=(P(("rep", "ep"), "tp"), P()),
        check_vma=False,
    )
```

```python
import functools

import jax
import jax.numpy as jnp
from jax import lax
from jax.experimental import pallas as pl
from jax.experimental.pallas import tpu as pltpu
from jax.sharding import PartitionSpec as P

REPL = 4
LANES = 128
PIECES = 2
MIB = 1 << 20

route_scale = 2.5


def shift(array, axis, count, step):
    return lax.ppermute(array, axis, [(i, (i + step) % count) for i in range(count)])


def swap(array, axis, count, span):
    return lax.ppermute(array, axis, [(i, i ^ span) for i in range(count)])


def window(index, size):
    return pl.ds(pl.multiple_of(index * size, size), size)


def copies_into(pairs, sems, pieces):
    copies = []
    for source, target in pairs:
        rows = target.shape[0] // pieces
        for piece in range(pieces):
            span = pl.ds(piece * rows, rows)
            copies.append(
                pltpu.make_async_copy(source.at[span], target.at[span], sems.at[len(copies)])
            )
    return copies


def first_kernel(ep_count, rep_count, ids_ref, picks_ref, gate_hbm, up_hbm, *refs):
    gate_out, up_out, counts_ref, sems = refs
    rows = window(lax.axis_index("tp"), gate_out.shape[0])
    copies = copies_into([(gate_hbm.at[rows], gate_out), (up_hbm.at[rows], up_out)], sems, PIECES)
    for copy in copies:
        copy.start()
    target = lax.axis_index("rep") + picks_ref[...] * (rep_count // REPL)
    cells = lax.rem(target, rep_count) * ep_count + ids_ref[...]
    rows, lanes = counts_ref.shape
    position = lax.broadcasted_iota(jnp.int32, (rows, lanes), 0) * lanes
    position = position + lax.broadcasted_iota(jnp.int32, (rows, lanes), 1)
    total = jnp.zeros((rows, lanes), jnp.int32)
    for k in range(cells.shape[0]):
        for t in range(cells.shape[1]):
            total += (position == cells[k : k + 1, t : t + 1]).astype(jnp.int32)
    counts_ref[...] = total
    for copy in copies:
        copy.wait()


def stack_kernel(*refs):
    pieces, out_ref = refs[:-2], refs[-1]
    for s, piece in enumerate(pieces):
        out_ref[pl.ds(s * piece.shape[0], piece.shape[0]), :] = piece[...]


def own_kernel(tp_count, *refs):
    x_ref, gate_ref, up_ref, gate_hbm, up_hbm, down_hbm = refs[:6]
    gate_acc, up_acc, gate_rest, up_rest, down_out, sems = refs[6:]
    part = x_ref.shape[1]
    me = lax.axis_index("tp")
    pairs = []
    for step in range(1, tp_count):
        rows = window(lax.rem(me - step + tp_count, tp_count), part)
        held = pl.ds((step - 1) * part, part)
        pairs.append((gate_hbm.at[rows], gate_rest.at[held]))
        pairs.append((up_hbm.at[rows], up_rest.at[held]))
    pairs.append((down_hbm, down_out))
    copies = copies_into(pairs, sems, PIECES)
    for copy in copies:
        copy.start()
    x = x_ref[...]
    gate_acc[...] = jnp.dot(x, gate_ref[...], preferred_element_type=jnp.float32)
    up_acc[...] = jnp.dot(x, up_ref[...], preferred_element_type=jnp.float32)
    for copy in copies:
        copy.wait()


def hidden_kernel(tp_count, *refs):
    others = refs[: tp_count - 1]
    gate_acc, up_acc, gate_ref, up_ref, down_ref = refs[tp_count - 1 : tp_count + 4]
    hidden_out = refs[tp_count + 4]
    partial_outs = refs[tp_count + 5 :]
    me = lax.axis_index("tp")
    gate = gate_acc[...]
    up = up_acc[...]
    for step, other in enumerate(others):
        rows = pl.ds(step * other.shape[1], other.shape[1])
        x = other[...]
        gate += jnp.dot(x, gate_ref[rows, :], preferred_element_type=jnp.float32)
        up += jnp.dot(x, up_ref[rows, :], preferred_element_type=jnp.float32)
    hidden = (gate / (1.0 + jnp.exp(-gate)) * up).astype(jnp.bfloat16)
    hidden_out[...] = hidden
    for step, out in enumerate(partial_outs, 1):
        columns = window(lax.rem(me + step, tp_count), out.shape[1])
        out[...] = jnp.dot(
            hidden, down_ref[:, columns], preferred_element_type=jnp.float32
        ).astype(jnp.bfloat16)


def down_kernel(hidden_ref, down_ref, counts_ref, swapped_ref, out_ref, sum_ref):
    sum_ref[...] = counts_ref[...] + swapped_ref[...]
    columns = window(lax.axis_index("tp"), out_ref.shape[1])
    out_ref[...] = jnp.dot(
        hidden_ref[...], down_ref[:, columns], preferred_element_type=jnp.float32
    )


def pack_kernel(arrived_count, *refs):
    mine_ref = refs[0]
    arrived = refs[1 : 1 + arrived_count]
    counts = refs[1 + arrived_count : 3 + arrived_count]
    outs = refs[3 + arrived_count :]
    tok_rows, part = outs[0].shape[0], mine_ref.shape[1]
    carried = (counts[0][...] + counts[1][...]).astype(jnp.float32).astype(jnp.bfloat16)
    for s, out in enumerate(outs):
        rows = pl.ds(s * tok_rows, tok_rows)
        total = mine_ref[rows, :]
        for piece in arrived:
            total += piece[rows, :].astype(jnp.float32)
        out[:, :part] = total.astype(jnp.bfloat16)
        out[:, part:] = carried


def combine_kernel(ep_count, ids_ref, scores_ref, *refs):
    pieces, (out_ref, counts_ref) = refs[:-2], refs[-2:]
    tok_rows, part = out_ref.shape
    me = lax.axis_index("ep")
    gains = jax.nn.sigmoid(scores_ref[...])
    weights = gains / jnp.sum(gains, 0, keepdims=True) * route_scale
    ids = ids_ref[...]
    total = jnp.zeros((tok_rows, part), jnp.float32)
    counts = jnp.zeros(counts_ref.shape, jnp.float32)
    diagonal = lax.broadcasted_iota(jnp.int32, (tok_rows, tok_rows), 0) == (
        lax.broadcasted_iota(jnp.int32, (tok_rows, tok_rows), 1)
    )
    for s, piece in enumerate(pieces):
        expert = lax.rem(me + s, ep_count)
        row = jnp.sum(jnp.where(ids == expert, weights, 0.0), 0, keepdims=True)
        column = jnp.sum(jnp.where(diagonal, row, 0.0), 1, keepdims=True)
        total += column * piece[:, :part].astype(jnp.float32)
        counts += piece[:, part:].astype(jnp.float32)
    out_ref[...] = total.astype(jnp.bfloat16)
    counts_ref[...] = counts.astype(jnp.int32)


def vmem_call(kernel, name, outs, args, flops, remote=0, copies=0):
    specs = [pl.BlockSpec(memory_space=pltpu.VMEM)] * (len(args) - remote)
    return pl.pallas_call(
        kernel,
        out_shape=[pltpu.VMEM(shape, dtype) for shape, dtype in outs],
        in_specs=specs + [pl.BlockSpec(memory_space=pltpu.HBM)] * remote,
        out_specs=[pl.BlockSpec(memory_space=pltpu.VMEM)] * len(outs),
        scratch_shapes=[pltpu.SemaphoreType.DMA((copies,))] if copies else [],
        compiler_params=pltpu.CompilerParams(vmem_limit_bytes=24 * MIB),
        cost_estimate=pl.CostEstimate(flops=flops, bytes_accessed=MIB, transcendentals=0),
        name=name,
    )(*args)


def per_device(tokens, expert_ids, replicas, scores, w_gate, w_up, w_down):
    rep_count = lax.axis_size("rep")
    ep_count = lax.axis_size("ep")
    tp_count = lax.axis_size("tp")
    tok_rows, part = tokens.shape
    ffe = w_gate.shape[2]
    rows = ep_count * tok_rows
    bf16, f32, i32 = jnp.bfloat16, jnp.float32, jnp.int32
    gate_w, up_w, down_w = (
        pltpu.with_memory_space_constraint(w[0], pltpu.HBM) for w in (w_gate, w_up, w_down)
    )
    ids, picks, gains = expert_ids.T, replicas.T, scores.T

    blocks = [tokens] + [shift(tokens, "ep", ep_count, s) for s in range(1, ep_count)]

    cell_count = rep_count * ep_count
    width = -(-cell_count // (tok_rows * LANES)) * LANES
    table = ((tok_rows, width), i32)
    gate_own, up_own, counts = vmem_call(
        functools.partial(first_kernel, ep_count, rep_count),
        "first_weights",
        [((part, ffe), bf16)] * 2 + [table],
        (ids, picks, gate_w, up_w),
        10**8,
        remote=2,
        copies=2 * PIECES,
    )
    (own,) = vmem_call(stack_kernel, "stack", [((rows, part), bf16)], (*blocks, counts), 1000)
    others = [shift(own, "tp", tp_count, s) for s in range(1, tp_count)]
    spans = [1 << bit for bit in range(rep_count.bit_length() - 1)]
    for span in spans[:-1]:
        swapped = swap(counts, "rep", rep_count, span)
        if span != spans[-2]:
            counts = counts + swapped
    dot_flops = 2 * rows * part * ffe
    rest = ((tp_count - 1) * part, ffe)
    gate_acc, up_acc, gate_rest, up_rest, down = vmem_call(
        functools.partial(own_kernel, tp_count),
        "own_features",
        [((rows, ffe), f32)] * 2 + [(rest, bf16)] * 2 + [(down_w.shape, bf16)],
        (own, gate_own, up_own, gate_w, up_w, down_w),
        2 * dot_flops,
        remote=3,
        copies=(2 * tp_count - 1) * PIECES,
    )
    hidden, *partials = vmem_call(
        functools.partial(hidden_kernel, tp_count),
        "hidden",
        [((rows, ffe), bf16)] + [((rows, part), bf16)] * (tp_count - 1),
        (*others, gate_acc, up_acc, gate_rest, up_rest, down),
        3 * (tp_count - 1) * dot_flops,
    )
    arrived = [shift(p, "tp", tp_count, s) for s, p in enumerate(partials, 1)]
    mine, counts = vmem_call(
        down_kernel,
        "own_down",
        [((rows, part), f32), table],
        (hidden, down, counts, swapped),
        dot_flops,
    )
    swapped = swap(counts, "rep", rep_count, spans[-1])

    outgoing = vmem_call(
        functools.partial(pack_kernel, tp_count - 1),
        "pack",
        [((tok_rows, part + width), bf16)] * ep_count,
        (mine, *arrived, counts, swapped),
        rows * part,
    )
    back = [outgoing[0]] + [
        shift(outgoing[s], "ep", ep_count, -s) for s in range(1, ep_count)
    ]
    moe_out, totals = pl.pallas_call(
        functools.partial(combine_kernel, ep_count),
        out_shape=[
            jax.ShapeDtypeStruct((tok_rows, part), bf16),
            jax.ShapeDtypeStruct((tok_rows, width), i32),
        ],
        compiler_params=pltpu.CompilerParams(vmem_limit_bytes=8 * MIB),
        name="combine",
    )(ids, gains, *back)
    load_counts = totals.reshape(-1)[:cell_count].reshape(rep_count, ep_count)
    return moe_out, load_counts


def solution(mesh):
    placed = (
        P(("rep", "ep"), "tp"),
        P(("rep", "ep"), None),
        P(("rep", "ep"), None),
        P(("rep", "ep"), None),
        P("ep", None, "tp"),
        P("ep", None, "tp"),
        P("ep", "tp", None),
    )
    return jax.shard_map(
        per_device,
        mesh=mesh,
        in_specs=placed,
        out_specs=(P(("rep", "ep"), "tp"), P()),
        check_vma=False,
    )
```

```python
import functools

import jax
import jax.numpy as jnp
from jax import lax
from jax.experimental import pallas as pl
from jax.experimental.pallas import tpu as pltpu
from jax.sharding import PartitionSpec as P

REPL = 4
LANES = 128
MIB = 1 << 20

route_scale = 2.5


def shift(array, axis, count, step):
    return lax.ppermute(array, axis, [(i, (i + step) % count) for i in range(count)])


def swap(array, axis, count, span):
    return lax.ppermute(array, axis, [(i, i ^ span) for i in range(count)])


def window(index, size):
    return pl.ds(pl.multiple_of(index * size, size), size)


def intake_kernel(ep_count, rep_count, tokens_hbm, ids_hbm, picks_hbm, *refs):
    tokens_out, counts_ref, ids_ref, picks_ref, sems = refs
    pairs = [(ids_hbm, ids_ref), (picks_hbm, picks_ref), (tokens_hbm, tokens_out)]
    copies = [
        pltpu.make_async_copy(source, held, sems.at[i]) for i, (source, held) in enumerate(pairs)
    ]
    for copy in copies:
        copy.start()
    for copy in copies:
        copy.wait()
    group = lax.rem(lax.axis_index("rep") + picks_ref[...] * (rep_count // REPL), rep_count)
    ids = ids_ref[...]
    rows, lanes = counts_ref.shape
    lane = (group // rows) * LANES + ids
    row = lax.rem(group, rows)
    cells = row * lanes + lane
    position = lax.broadcasted_iota(jnp.int32, (rows, lanes), 0) * lanes
    position = position + lax.broadcasted_iota(jnp.int32, (rows, lanes), 1)
    total = jnp.zeros((rows, lanes), jnp.int32)
    for k in range(cells.shape[0]):
        for t in range(cells.shape[1]):
            total += (position == cells[k : k + 1, t : t + 1]).astype(jnp.int32)
    counts_ref[...] = total


def stack_kernel(*refs):
    pieces, out_ref = refs[:-1], refs[-1]
    for s, piece in enumerate(pieces):
        out_ref[pl.ds(s * piece.shape[0], piece.shape[0]), :] = piece[...]


def own_kernel(x_ref, gate_ref, up_ref, gate_acc, up_acc):
    rows = window(lax.axis_index("tp"), x_ref.shape[1])
    x = x_ref[...]
    gate_acc[...] = jnp.dot(x, gate_ref[rows, :], preferred_element_type=jnp.float32)
    up_acc[...] = jnp.dot(x, up_ref[rows, :], preferred_element_type=jnp.float32)


def hidden_kernel(tp_count, *refs):
    others = refs[: tp_count - 1]
    gate_acc, up_acc, gate_ref, up_ref, down_ref = refs[tp_count - 1 : tp_count + 4]
    hidden_out = refs[tp_count + 4]
    partial_outs = refs[tp_count + 5 :]
    me = lax.axis_index("tp")
    gate = gate_acc[...]
    up = up_acc[...]
    for step, other in enumerate(others, 1):
        rows = window(lax.rem(me - step + tp_count, tp_count), other.shape[1])
        x = other[...]
        gate += jnp.dot(x, gate_ref[rows, :], preferred_element_type=jnp.float32)
        up += jnp.dot(x, up_ref[rows, :], preferred_element_type=jnp.float32)
    hidden = (gate / (1.0 + jnp.exp(-gate)) * up).astype(jnp.bfloat16)
    hidden_out[...] = hidden
    for step, out in enumerate(partial_outs, 1):
        columns = window(lax.rem(me + step, tp_count), out.shape[1])
        out[...] = jnp.dot(
            hidden, down_ref[:, columns], preferred_element_type=jnp.float32
        ).astype(jnp.bfloat16)


def down_kernel(hidden_ref, down_ref, counts_ref, swapped_ref, out_ref, sum_ref):
    sum_ref[...] = counts_ref[...] + swapped_ref[...]
    columns = window(lax.axis_index("tp"), out_ref.shape[1])
    out_ref[...] = jnp.dot(
        hidden_ref[...], down_ref[:, columns], preferred_element_type=jnp.float32
    )


def pack_kernel(arrived_count, *refs):
    mine_ref = refs[0]
    arrived = refs[1 : 1 + arrived_count]
    counts = refs[1 + arrived_count : 3 + arrived_count]
    outs = refs[3 + arrived_count :]
    tok_rows, part = outs[0].shape[0], mine_ref.shape[1]
    carried = (counts[0][...] + counts[1][...]).astype(jnp.float32).astype(jnp.bfloat16)
    for s, out in enumerate(outs):
        rows = pl.ds(s * tok_rows, tok_rows)
        total = mine_ref[rows, :]
        for piece in arrived:
            total += piece[rows, :].astype(jnp.float32)
        out[:, :part] = total.astype(jnp.bfloat16)
        out[:, part:] = carried


def combine_kernel(ep_count, ids_ref, scores_ref, *refs):
    pieces, (out_ref, counts_ref) = refs[:-2], refs[-2:]
    tok_rows, part = out_ref.shape
    me = lax.axis_index("ep")
    gains = jax.nn.sigmoid(scores_ref[...])
    weights = gains / jnp.sum(gains, 0, keepdims=True) * route_scale
    ids = ids_ref[...]
    total = jnp.zeros((tok_rows, part), jnp.float32)
    counts = jnp.zeros((tok_rows, pieces[0].shape[1] - part), jnp.float32)
    diagonal = lax.broadcasted_iota(jnp.int32, (tok_rows, tok_rows), 0) == (
        lax.broadcasted_iota(jnp.int32, (tok_rows, tok_rows), 1)
    )
    for s, piece in enumerate(pieces):
        expert = lax.rem(me + s, ep_count)
        row = jnp.sum(jnp.where(ids == expert, weights, 0.0), 0, keepdims=True)
        column = jnp.sum(jnp.where(diagonal, row, 0.0), 1, keepdims=True)
        total += column * piece[:, :part].astype(jnp.float32)
        counts += piece[:, part:].astype(jnp.float32)
    out_ref[...] = total.astype(jnp.bfloat16)
    for group in range(0, counts_ref.shape[0], tok_rows):
        size = min(tok_rows, counts_ref.shape[0] - group)
        start = group // tok_rows * LANES
        counts_ref[pl.ds(group, size), :] = counts[:size, start : start + ep_count].astype(jnp.int32)


def vmem_call(kernel, name, outs, args, flops, remote=0, scratch=()):
    specs = [pl.BlockSpec(memory_space=pltpu.VMEM)] * (len(args) - remote)
    return pl.pallas_call(
        kernel,
        out_shape=[pltpu.VMEM(shape, dtype) for shape, dtype in outs],
        in_specs=specs + [pl.BlockSpec(memory_space=pltpu.HBM)] * remote,
        out_specs=[pl.BlockSpec(memory_space=pltpu.VMEM)] * len(outs),
        scratch_shapes=list(scratch),
        compiler_params=pltpu.CompilerParams(vmem_limit_bytes=24 * MIB),
        cost_estimate=pl.CostEstimate(flops=flops, bytes_accessed=MIB, transcendentals=0),
        name=name,
    )(*args)


def per_device(tokens, expert_ids, replicas, scores, w_gate, w_up, w_down):
    rep_count = lax.axis_size("rep")
    ep_count = lax.axis_size("ep")
    tp_count = lax.axis_size("tp")
    tok_rows, part = tokens.shape
    ffe = w_gate.shape[2]
    rows = ep_count * tok_rows
    bf16, f32, i32 = jnp.bfloat16, jnp.float32, jnp.int32
    gate_w, up_w, down_w = w_gate[0], w_up[0], w_down[0]
    ids, picks, gains = expert_ids.T, replicas.T, scores.T

    width = -(-rep_count // tok_rows) * LANES
    table = ((tok_rows, width), i32)
    tokens, counts = vmem_call(
        functools.partial(intake_kernel, ep_count, rep_count),
        "intake",
        [((tok_rows, part), bf16), table],
        tuple(pltpu.with_memory_space_constraint(a, pltpu.HBM) for a in (tokens, ids, picks)),
        10**11,
        remote=3,
        scratch=[pltpu.VMEM(ids.shape, i32)] * 2 + [pltpu.SemaphoreType.DMA((3,))],
    )

    blocks = [tokens] + [shift(tokens, "ep", ep_count, s) for s in range(1, ep_count)]
    (own,) = vmem_call(stack_kernel, "stack", [((rows, part), bf16)], tuple(blocks), 1000)
    others = [shift(own, "tp", tp_count, s) for s in range(1, tp_count)]
    spans = [1 << bit for bit in range(rep_count.bit_length() - 1)]
    for span in spans[:-1]:
        swapped = swap(counts, "rep", rep_count, span)
        if span != spans[-2]:
            counts = counts + swapped
    dot_flops = 2 * rows * part * ffe
    gate_acc, up_acc = vmem_call(
        own_kernel,
        "own_features",
        [((rows, ffe), f32)] * 2,
        (own, gate_w, up_w),
        2 * dot_flops,
    )
    hidden, *partials = vmem_call(
        functools.partial(hidden_kernel, tp_count),
        "hidden",
        [((rows, ffe), bf16)] + [((rows, part), bf16)] * (tp_count - 1),
        (*others, gate_acc, up_acc, gate_w, up_w, down_w),
        3 * (tp_count - 1) * dot_flops,
    )
    arrived = [shift(p, "tp", tp_count, s) for s, p in enumerate(partials, 1)]
    mine, counts = vmem_call(
        down_kernel,
        "own_down",
        [((rows, part), f32), table],
        (hidden, down_w, counts, swapped),
        dot_flops,
    )
    swapped = swap(counts, "rep", rep_count, spans[-1])

    outgoing = vmem_call(
        functools.partial(pack_kernel, tp_count - 1),
        "pack",
        [((tok_rows, part + width), bf16)] * ep_count,
        (mine, *arrived, counts, swapped),
        rows * part,
    )
    back = [outgoing[0]] + [
        shift(outgoing[s], "ep", ep_count, -s) for s in range(1, ep_count)
    ]
    return pl.pallas_call(
        functools.partial(combine_kernel, ep_count),
        out_shape=[
            jax.ShapeDtypeStruct((tok_rows, part), bf16),
            jax.ShapeDtypeStruct((rep_count, ep_count), i32),
        ],
        compiler_params=pltpu.CompilerParams(vmem_limit_bytes=8 * MIB),
        name="combine",
    )(ids, gains, *back)


def solution(mesh):
    placed = (
        P(("rep", "ep"), "tp"),
        P(("rep", "ep"), None),
        P(("rep", "ep"), None),
        P(("rep", "ep"), None),
        P("ep", None, "tp"),
        P("ep", None, "tp"),
        P("ep", "tp", None),
    )
    return jax.shard_map(
        per_device,
        mesh=mesh,
        in_specs=placed,
        out_specs=(P(("rep", "ep"), "tp"), P()),
        check_vma=False,
    )
```

```python
import functools

import jax
import jax.numpy as jnp
from jax import lax
from jax.experimental import pallas as pl
from jax.experimental.pallas import tpu as pltpu
from jax.sharding import PartitionSpec as P

REPL = 4
LANES = 128
MIB = 1 << 20

route_scale = 2.5


def shift(array, axis, count, step):
    return lax.ppermute(array, axis, [(i, (i + step) % count) for i in range(count)])


def swap(array, axis, count, span):
    return lax.ppermute(array, axis, [(i, i ^ span) for i in range(count)])


def window(index, size):
    return pl.ds(pl.multiple_of(index * size, size), size)


def dot(a, b):
    return jnp.dot(a, b, preferred_element_type=jnp.float32)


def ready_kernel(out_ref):
    out_ref[...] = jnp.zeros(out_ref.shape, out_ref.dtype)


def intake_kernel(rep_count, tokens_ref, ids_ref, picks_ref, ready_ref, out_ref):
    part = tokens_ref.shape[1]
    group = lax.rem(lax.axis_index("rep") + picks_ref[...] * (rep_count // REPL), rep_count)
    ids = ids_ref[...]
    rows, lanes = out_ref.shape[0], out_ref.shape[1] - part
    cells = lax.rem(group, rows) * lanes + (group // rows) * LANES + ids
    position = lax.broadcasted_iota(jnp.int32, (rows, lanes), 0) * lanes
    position = position + lax.broadcasted_iota(jnp.int32, (rows, lanes), 1)
    total = jnp.zeros((rows, lanes), jnp.float32)
    for k in range(cells.shape[0]):
        for t in range(cells.shape[1]):
            total += (position == cells[k : k + 1, t : t + 1]).astype(jnp.float32)
    out_ref[:, :part] = tokens_ref[...]
    out_ref[:, part:] = total.astype(out_ref.dtype)


def stack_kernel(*refs):
    pieces, out_ref = refs[:-1], refs[-1]
    tok_rows, part = pieces[0].shape[0], out_ref.shape[1]
    for s, piece in enumerate(pieces):
        out_ref[pl.ds(s * tok_rows, tok_rows), :] = piece[:, :part]


def sum_kernel(*refs):
    pieces, out_ref = refs[:-1], refs[-1]
    part = pieces[0].shape[1] - out_ref.shape[1]
    out_ref[...] = sum(piece[:, part:].astype(jnp.float32) for piece in pieces).astype(jnp.int32)


def joined(refs):
    return jnp.concatenate([ref[...] for ref in refs], 0)


def own_kernel(*refs):
    pieces, (gate_ref, up_ref, down_ref, gate_acc, up_acc) = refs[:-5], refs[-5:]
    rows = window(lax.axis_index("tp"), pieces[0].shape[1])
    x = joined(pieces)
    gate_acc[...] = dot(x, gate_ref[rows, :])
    up_acc[...] = dot(x, up_ref[rows, :])


def hidden_kernel(tp_count, group_count, places, *refs):
    total = (tp_count - 1) * group_count
    others, refs = refs[:total], refs[total:]
    (gate_acc, up_acc, gate_ref, up_ref, down_ref, hidden_out), outs = refs[:6], refs[6:]
    me = lax.axis_index("tp")
    part = others[0].shape[1]
    gate = gate_acc[...]
    up = up_acc[...]
    for step in range(1, tp_count):
        rows = window(lax.rem(me - step + tp_count, tp_count), part)
        x = joined(others[(step - 1) * group_count : step * group_count])
        gate += dot(x, gate_ref[rows, :])
        up += dot(x, up_ref[rows, :])
    hidden = (gate / (1.0 + jnp.exp(-gate)) * up).astype(jnp.bfloat16)
    hidden_out[...] = hidden
    for step in range(1, tp_count):
        columns = window(lax.rem(me + step, tp_count), part)
        partial = dot(hidden, down_ref[:, columns]).astype(jnp.bfloat16)
        for place, out in zip(places, outs[(step - 1) * len(places) :]):
            size = out.shape[0] // len(place)
            for i, p in enumerate(place):
                out[pl.ds(i * size, size), :] = partial[p * size : (p + 1) * size]


def down_kernel(hidden_ref, down_ref, out_ref):
    columns = window(lax.axis_index("tp"), out_ref.shape[1])
    out_ref[...] = dot(hidden_ref[...], down_ref[:, columns])


def pack_kernel(place, arrived_count, mine_ref, *refs):
    arrived, outs = refs[:arrived_count], refs[arrived_count:]
    size = outs[0].shape[0]
    for i, (p, out) in enumerate(zip(place, outs)):
        total = mine_ref[pl.ds(p * size, size), :]
        for piece in arrived:
            total += piece[pl.ds(i * size, size), :].astype(jnp.float32)
        out[...] = total.astype(jnp.bfloat16)


def combine_kernel(ids_ref, scores_ref, sum_ref, swapped_ref, *refs):
    pieces, (out_ref, counts_ref) = refs[:-2], refs[-2:]
    ep_count = len(pieces)
    tok_rows, part = out_ref.shape
    me = lax.axis_index("ep")
    gains = jax.nn.sigmoid(scores_ref[...])
    weights = gains / jnp.sum(gains, 0, keepdims=True) * route_scale
    ids = ids_ref[...]
    total = jnp.zeros((tok_rows, part), jnp.float32)
    diagonal = lax.broadcasted_iota(jnp.int32, (tok_rows, tok_rows), 0) == (
        lax.broadcasted_iota(jnp.int32, (tok_rows, tok_rows), 1)
    )
    for s, piece in enumerate(pieces):
        row = jnp.sum(jnp.where(ids == (me ^ s), weights, 0.0), 0, keepdims=True)
        column = jnp.sum(jnp.where(diagonal, row, 0.0), 1, keepdims=True)
        total += column * piece[...].astype(jnp.float32)
    out_ref[...] = total.astype(jnp.bfloat16)
    counts = sum_ref[...] + swapped_ref[...]
    for group in range(0, counts_ref.shape[0], tok_rows):
        size = min(tok_rows, counts_ref.shape[0] - group)
        start = group // tok_rows * LANES
        counts_ref[pl.ds(group, size), :] = counts[:size, start : start + ep_count]


def vmem_call(kernel, outs, args, flops):
    return pl.pallas_call(
        kernel,
        out_shape=[pltpu.VMEM(shape, dtype) for shape, dtype in outs],
        in_specs=[pl.BlockSpec(memory_space=pltpu.VMEM)] * len(args),
        out_specs=[pl.BlockSpec(memory_space=pltpu.VMEM)] * len(outs),
        compiler_params=pltpu.CompilerParams(vmem_limit_bytes=24 * MIB),
        cost_estimate=pl.CostEstimate(flops=flops, bytes_accessed=MIB, transcendentals=0),
    )(*args)


def per_device(tokens, expert_ids, replicas, scores, w_gate, w_up, w_down):
    rep_count = lax.axis_size("rep")
    ep_count = lax.axis_size("ep")
    tp_count = lax.axis_size("tp")
    tok_rows, part = tokens.shape
    ffe = w_gate.shape[2]
    rows = ep_count * tok_rows
    groups, out_groups = row_groups(ep_count)
    order = [s for group in groups for s in group]
    places = [[order.index(s) for s in group] for group in out_groups]
    bf16, f32, i32 = jnp.bfloat16, jnp.float32, jnp.int32
    gate_w, up_w, down_w = w_gate[0], w_up[0], w_down[0]

    ids, picks, gains = expert_ids.T, replicas.T, scores.T

    (ready,) = vmem_call(ready_kernel, [((8, LANES), f32)], (), 10**11)

    width = -(-rep_count // tok_rows) * LANES
    (message,) = vmem_call(
        functools.partial(intake_kernel, rep_count),
        [((tok_rows, part + width), bf16)],
        (tokens, ids, picks, ready),
        1000,
    )

    blocks = [message]
    blocks += [swap(message, "ep", ep_count, s) for s in range(1, ep_count)]
    steps = range(1, tp_count)
    owned, others = [], []
    for group in groups:
        shape = (len(group) * tok_rows, part)
        held = tuple(blocks[s] for s in group)
        owned += vmem_call(stack_kernel, [(shape, bf16)], held, 1000)
        others.append([shift(owned[-1], "tp", tp_count, s) for s in steps])
    (counts,) = vmem_call(sum_kernel, [((tok_rows, width), i32)], tuple(blocks), 1000)
    swapped = jnp.zeros_like(counts)
    for bit in range(rep_count.bit_length() - 1):
        counts = counts + swapped
        swapped = swap(counts, "rep", rep_count, 1 << bit)
    dot_flops = 2 * rows * part * ffe
    gate_acc, up_acc = vmem_call(
        own_kernel, [((rows, ffe), f32)] * 2, (*owned, gate_w, up_w, down_w), 2 * dot_flops
    )
    hidden, *partials = vmem_call(
        functools.partial(hidden_kernel, tp_count, len(groups), places),
        [((rows, ffe), bf16)]
        + [((len(p) * tok_rows, part), bf16) for p in places] * len(steps),
        (*[group[s - 1] for s in steps for group in others], gate_acc, up_acc, gate_w, up_w, down_w),
        3 * len(steps) * dot_flops,
    )
    arrived = []
    for number in range(len(places)):
        pieces = partials[number :: len(places)]
        arrived.append([shift(p, "tp", tp_count, s) for s, p in zip(steps, pieces)])
    (mine,) = vmem_call(down_kernel, [((rows, part), f32)], (hidden, down_w), dot_flops)

    back = [None] * ep_count
    for number, group in enumerate(out_groups):
        outgoing = vmem_call(
            functools.partial(pack_kernel, places[number], len(steps)),
            [((tok_rows, part), bf16)] * len(group),
            (mine, *arrived[number]),
            1000,
        )
        for s, piece in zip(group, outgoing):
            back[s] = swap(piece, "ep", ep_count, s) if s else piece
    return pl.pallas_call(
        combine_kernel,
        out_shape=[
            jax.ShapeDtypeStruct((tok_rows, part), bf16),
            jax.ShapeDtypeStruct((rep_count, ep_count), i32),
        ],
        compiler_params=pltpu.CompilerParams(vmem_limit_bytes=8 * MIB),
        name="combine",
    )(ids, gains, counts, swapped, *back)


def row_groups(ep_count):
    half = ep_count // 2
    far = list(range(ep_count - 1, half, -1))
    near = list(range(1, half))
    return [[0, half], far + near], [[half], far, near + [0]]


def solution(mesh):
    placed = (
        P(("rep", "ep"), "tp"),
        P(("rep", "ep"), None),
        P(("rep", "ep"), None),
        P(("rep", "ep"), None),
        P("ep", None, "tp"),
        P("ep", None, "tp"),
        P("ep", "tp", None),
    )

    return jax.shard_map(
        per_device,
        mesh=mesh,
        in_specs=placed,
        out_specs=(P(("rep", "ep"), "tp"), P()),
        check_vma=False,
    )
```

```python
import functools

import jax
import jax.numpy as jnp
from jax import lax
from jax.experimental import pallas as pl
from jax.experimental.pallas import tpu as pltpu
from jax.sharding import PartitionSpec as P

REPL = 4
LANES = 128
MIB = 1 << 20

route_scale = 2.5


def shift(array, axis, count, step):
    return lax.ppermute(array, axis, [(i, (i + step) % count) for i in range(count)])


def swap(array, axis, count, span):
    return lax.ppermute(array, axis, [(i, i ^ span) for i in range(count)])


def diagonal(array, ep_count, tp_count, span, step):
    pairs = [
        (e * tp_count + t, (e ^ span) * tp_count + (t + step) % tp_count)
        for e in range(ep_count)
        for t in range(tp_count)
    ]
    return lax.ppermute(array, ("ep", "tp"), pairs)


def window(index, size):
    return pl.ds(pl.multiple_of(index * size, size), size)


def dot(a, b):
    return jnp.dot(a, b, preferred_element_type=jnp.float32)


def ready_kernel(out_ref):
    out_ref[...] = jnp.zeros(out_ref.shape, out_ref.dtype)


def intake_kernel(rep_count, tokens_ref, ids_ref, picks_ref, ready_ref, out_ref):
    part = tokens_ref.shape[1]
    group = lax.rem(lax.axis_index("rep") + picks_ref[...] * (rep_count // REPL), rep_count)
    ids = ids_ref[...]
    rows, lanes = out_ref.shape[0], out_ref.shape[1] - part
    cells = lax.rem(group, rows) * lanes + (group // rows) * LANES + ids
    position = lax.broadcasted_iota(jnp.int32, (rows, lanes), 0) * lanes
    position = position + lax.broadcasted_iota(jnp.int32, (rows, lanes), 1)
    total = jnp.zeros((rows, lanes), jnp.float32)
    for k in range(cells.shape[0]):
        for t in range(cells.shape[1]):
            total += (position == cells[k : k + 1, t : t + 1]).astype(jnp.float32)
    out_ref[:, :part] = tokens_ref[...]
    out_ref[:, part:] = total.astype(out_ref.dtype)


def stack_kernel(*refs):
    pieces, outs = refs[:-2], refs[-2:]
    tok_rows, size = pieces[0].shape[0], outs[0].shape[1]
    for s, piece in enumerate(pieces):
        for h, out in enumerate(outs):
            out[pl.ds(s * tok_rows, tok_rows), :] = piece[:, h * size : (h + 1) * size]


def sum_kernel(*refs):
    pieces, out_ref = refs[:-1], refs[-1]
    part = pieces[0].shape[1] - out_ref.shape[1]
    out_ref[...] = sum(piece[:, part:].astype(jnp.float32) for piece in pieces).astype(jnp.int32)


def slab(split_ref, whole_refs, h):
    size = split_ref.shape[1]
    pieces = [split_ref[...]] + [ref[:, h * size : (h + 1) * size] for ref in whole_refs]
    return jnp.concatenate(pieces, 0)


def own_kernel(*refs):
    splits, pieces = refs[:2], refs[2:-5]
    gate_ref, up_ref, _, gate_acc, up_acc = refs[-5:]
    size = splits[0].shape[1]
    gate, up = 0.0, 0.0
    for h, split in enumerate(splits):
        rows = window(lax.axis_index("tp") * 2 + h, size)
        x = slab(split, pieces, h)
        gate += dot(x, gate_ref[rows, :])
        up += dot(x, up_ref[rows, :])
    gate_acc[...] = gate
    up_acc[...] = up


def other_features(tp_count, h, others, gate_ref, up_ref):
    me = lax.axis_index("tp")
    each = len(others) // (tp_count - 1)
    gate, up = 0.0, 0.0
    for step in range(1, tp_count):
        split, *whole = others[(step - 1) * each : step * each]
        rows = window(lax.rem(me - step + tp_count, tp_count) * 2 + h, split.shape[1])
        x = slab(split, whole, h)
        gate += dot(x, gate_ref[rows, :])
        up += dot(x, up_ref[rows, :])
    return gate, up


def early_kernel(tp_count, *refs):
    others, (gate_ref, up_ref, gate_acc, up_acc, gate_out, up_out) = refs[:-6], refs[-6:]
    gate, up = other_features(tp_count, 0, others, gate_ref, up_ref)
    gate_out[...] = gate_acc[...] + gate
    up_out[...] = up_acc[...] + up


def hidden_kernel(tp_count, count, places, *refs):
    others, refs = refs[:count], refs[count:]
    (gate_acc, up_acc, gate_ref, up_ref, down_ref, hidden_out), outs = refs[:6], refs[6:]
    me = lax.axis_index("tp")
    part = gate_ref.shape[0] // tp_count
    gate, up = other_features(tp_count, 1, others, gate_ref, up_ref)
    gate += gate_acc[...]
    up += up_acc[...]
    hidden = (gate / (1.0 + jnp.exp(-gate)) * up).astype(jnp.bfloat16)
    hidden_out[...] = hidden
    for step in range(1, tp_count):
        columns = window(lax.rem(me + step, tp_count), part)
        partial = dot(hidden, down_ref[:, columns]).astype(jnp.bfloat16)
        for place, out in zip(places, outs[(step - 1) * len(places) :]):
            size = out.shape[0] // len(place)
            for i, p in enumerate(place):
                out[pl.ds(i * size, size), :] = partial[p * size : (p + 1) * size]


def down_kernel(hidden_ref, down_ref, out_ref):
    columns = window(lax.axis_index("tp"), out_ref.shape[1])
    out_ref[...] = dot(hidden_ref[...], down_ref[:, columns])


def pack_kernel(place, arrived_count, mine_ref, *refs):
    arrived, outs = refs[:arrived_count], refs[arrived_count:]
    size = outs[0].shape[0]
    for i, (p, out) in enumerate(zip(place, outs)):
        total = mine_ref[pl.ds(p * size, size), :]
        for piece in arrived:
            total += piece[pl.ds(i * size, size), :].astype(jnp.float32)
        out[...] = total.astype(jnp.bfloat16)


def combine_kernel(ids_ref, scores_ref, sum_ref, swapped_ref, *refs):
    pieces, (out_ref, counts_ref) = refs[:-2], refs[-2:]
    ep_count = len(pieces)
    tok_rows, part = out_ref.shape
    me = lax.axis_index("ep")
    gains = jax.nn.sigmoid(scores_ref[...])
    weights = gains / jnp.sum(gains, 0, keepdims=True) * route_scale
    ids = ids_ref[...]
    total = jnp.zeros((tok_rows, part), jnp.float32)
    diagonal = lax.broadcasted_iota(jnp.int32, (tok_rows, tok_rows), 0) == (
        lax.broadcasted_iota(jnp.int32, (tok_rows, tok_rows), 1)
    )
    for s, piece in enumerate(pieces):
        row = jnp.sum(jnp.where(ids == (me ^ s), weights, 0.0), 0, keepdims=True)
        column = jnp.sum(jnp.where(diagonal, row, 0.0), 1, keepdims=True)
        total += column * piece[...].astype(jnp.float32)
    out_ref[...] = total.astype(jnp.bfloat16)
    counts = sum_ref[...] + swapped_ref[...]
    for group in range(0, counts_ref.shape[0], tok_rows):
        size = min(tok_rows, counts_ref.shape[0] - group)
        start = group // tok_rows * LANES
        counts_ref[pl.ds(group, size), :] = counts[:size, start : start + ep_count]


def vmem_call(kernel, outs, args, flops):
    return pl.pallas_call(
        kernel,
        out_shape=[pltpu.VMEM(shape, dtype) for shape, dtype in outs],
        in_specs=[pl.BlockSpec(memory_space=pltpu.VMEM)] * len(args),
        out_specs=[pl.BlockSpec(memory_space=pltpu.VMEM)] * len(outs),
        compiler_params=pltpu.CompilerParams(vmem_limit_bytes=24 * MIB),
        cost_estimate=pl.CostEstimate(flops=flops, bytes_accessed=MIB, transcendentals=0),
    )(*args)


def per_device(tokens, expert_ids, replicas, scores, w_gate, w_up, w_down):
    rep_count = lax.axis_size("rep")
    ep_count = lax.axis_size("ep")
    tp_count = lax.axis_size("tp")
    tok_rows, part = tokens.shape
    ffe = w_gate.shape[2]
    rows = ep_count * tok_rows
    group, direct, out_groups = row_groups(ep_count)
    order = group + direct
    places = [[order.index(s) for s in group] for group in out_groups]
    bf16, f32, i32 = jnp.bfloat16, jnp.float32, jnp.int32
    gate_w, up_w, down_w = w_gate[0], w_up[0], w_down[0]

    ids, picks, gains = expert_ids.T, replicas.T, scores.T

    (ready,) = vmem_call(ready_kernel, [((8, LANES), f32)], (), 10**11)

    width = -(-rep_count // tok_rows) * LANES
    (message,) = vmem_call(
        functools.partial(intake_kernel, rep_count),
        [((tok_rows, part + width), bf16)],
        (tokens, ids, picks, ready),
        1000,
    )

    blocks = [message]
    blocks += [swap(message, "ep", ep_count, s) for s in range(1, ep_count)]
    steps = range(1, tp_count)
    shape = (len(group) * tok_rows, part // 2)
    halves = vmem_call(stack_kernel, [(shape, bf16)] * 2, tuple(blocks[s] for s in group), 1000)
    exchanged = []
    for held in halves:
        exchanged.append([shift(held, "tp", tp_count, d) for d in steps])
    across = []
    for s in direct:
        across.append([diagonal(tokens, ep_count, tp_count, s, d) for d in steps])
    others = [
        [ref for d in steps for ref in (exchanged[h][d - 1], *[a[d - 1] for a in across])]
        for h in range(2)
    ]
    (counts,) = vmem_call(sum_kernel, [((tok_rows, width), i32)], tuple(blocks), 1000)
    swapped = jnp.zeros_like(counts)
    for bit in range(rep_count.bit_length() - 1):
        counts = counts + swapped
        swapped = swap(counts, "rep", rep_count, 1 << bit)
    dot_flops = 2 * rows * part * ffe
    gate_acc, up_acc = vmem_call(
        own_kernel,
        [((rows, ffe), f32)] * 2,
        (*halves, *[blocks[s] for s in direct], gate_w, up_w, down_w),
        2 * dot_flops,
    )
    gate_acc, up_acc = vmem_call(
        functools.partial(early_kernel, tp_count),
        [((rows, ffe), f32)] * 2,
        (*others[0], gate_w, up_w, gate_acc, up_acc),
        dot_flops,
    )
    hidden, *partials = vmem_call(
        functools.partial(hidden_kernel, tp_count, len(others[1]), places),
        [((rows, ffe), bf16)]
        + [((len(p) * tok_rows, part), bf16) for p in places] * len(steps),
        (*others[1], gate_acc, up_acc, gate_w, up_w, down_w),
        3 * len(steps) * dot_flops,
    )
    arrived = []
    for number in range(len(places)):
        pieces = partials[number :: len(places)]
        arrived.append([shift(p, "tp", tp_count, s) for s, p in zip(steps, pieces)])
    (mine,) = vmem_call(down_kernel, [((rows, part), f32)], (hidden, down_w), dot_flops)

    back = [None] * ep_count
    for number, group in enumerate(out_groups):
        outgoing = vmem_call(
            functools.partial(pack_kernel, places[number], len(steps)),
            [((tok_rows, part), bf16)] * len(group),
            (mine, *arrived[number]),
            1000,
        )
        for s, piece in zip(group, outgoing):
            back[s] = swap(piece, "ep", ep_count, s) if s else piece
    return pl.pallas_call(
        combine_kernel,
        out_shape=[
            jax.ShapeDtypeStruct((tok_rows, part), bf16),
            jax.ShapeDtypeStruct((rep_count, ep_count), i32),
        ],
        compiler_params=pltpu.CompilerParams(vmem_limit_bytes=8 * MIB),
        name="combine",
    )(ids, gains, counts, swapped, *back)


def row_groups(ep_count):
    half = ep_count // 2
    far = list(range(ep_count - 1, half, -1))
    near = list(range(1, half))
    return [0, half] + near, far, [[half], far, near + [0]]


def solution(mesh):
    placed = (
        P(("rep", "ep"), "tp"),
        P(("rep", "ep"), None),
        P(("rep", "ep"), None),
        P(("rep", "ep"), None),
        P("ep", None, "tp"),
        P("ep", None, "tp"),
        P("ep", "tp", None),
    )

    return jax.shard_map(
        per_device,
        mesh=mesh,
        in_specs=placed,
        out_specs=(P(("rep", "ep"), "tp"), P()),
        check_vma=False,
    )
```

```python
import functools

import jax
import jax.numpy as jnp
from jax import lax
from jax.experimental import pallas as pl
from jax.experimental.pallas import tpu as pltpu
from jax.sharding import PartitionSpec as P

REPL = 4
LANES = 128
MIB = 1 << 20

route_scale = 2.5


def shift(array, axis, count, step):
    return lax.ppermute(array, axis, [(i, (i + step) % count) for i in range(count)])


def swap(array, axis, count, span):
    return lax.ppermute(array, axis, [(i, i ^ span) for i in range(count)])


def diagonal(array, ep_count, tp_count, span, step):
    pairs = [
        (e * tp_count + t, (e ^ span) * tp_count + (t + step) % tp_count)
        for e in range(ep_count)
        for t in range(tp_count)
    ]
    return lax.ppermute(array, ("ep", "tp"), pairs)


def window(index, size):
    return pl.ds(pl.multiple_of(index * size, size), size)


def dot(a, b):
    return jnp.dot(a, b, preferred_element_type=jnp.float32)


def ready_kernel(out_ref):
    out_ref[...] = jnp.zeros(out_ref.shape, out_ref.dtype)


def intake_kernel(rep_count, tokens_ref, ids_ref, picks_ref, ready_ref, out_ref):
    part = tokens_ref.shape[1]
    group = lax.rem(lax.axis_index("rep") + picks_ref[...] * (rep_count // REPL), rep_count)
    ids = ids_ref[...]
    rows, lanes = out_ref.shape[0], out_ref.shape[1] - part
    cells = lax.rem(group, rows) * lanes + (group // rows) * LANES + ids
    position = lax.broadcasted_iota(jnp.int32, (rows, lanes), 0) * lanes
    position = position + lax.broadcasted_iota(jnp.int32, (rows, lanes), 1)
    total = jnp.zeros((rows, lanes), jnp.float32)
    for k in range(cells.shape[0]):
        for t in range(cells.shape[1]):
            total += (position == cells[k : k + 1, t : t + 1]).astype(jnp.float32)
    out_ref[:, :part] = tokens_ref[...]
    out_ref[:, part:] = total.astype(out_ref.dtype)


def stack_kernel(*refs):
    pieces, outs = refs[:-2], refs[-2:]
    tok_rows, size = pieces[0].shape[0], outs[0].shape[1]
    for s, piece in enumerate(pieces):
        for h, out in enumerate(outs):
            out[pl.ds(s * tok_rows, tok_rows), :] = piece[:, h * size : (h + 1) * size]


def sum_kernel(*refs):
    pieces, out_ref = refs[:-1], refs[-1]
    part = pieces[0].shape[1] - out_ref.shape[1]
    out_ref[...] = sum(piece[:, part:].astype(jnp.float32) for piece in pieces).astype(jnp.int32)


def slab(split_ref, whole_refs, h):
    size = split_ref.shape[1]
    pieces = [split_ref[...]] + [ref[:, h * size : (h + 1) * size] for ref in whole_refs]
    return jnp.concatenate(pieces, 0)


def own_kernel(*refs):
    splits, pieces = refs[:2], refs[2:-5]
    gate_ref, up_ref, _, gate_acc, up_acc = refs[-5:]
    size = splits[0].shape[1]
    gate, up = 0.0, 0.0
    for h, split in enumerate(splits):
        rows = window(lax.axis_index("tp") * 2 + h, size)
        x = slab(split, pieces, h)
        gate += dot(x, gate_ref[rows, :])
        up += dot(x, up_ref[rows, :])
    gate_acc[...] = gate
    up_acc[...] = up


def other_features(tp_count, h, others, gate_ref, up_ref):
    me = lax.axis_index("tp")
    each = len(others) // (tp_count - 1)
    gate, up = 0.0, 0.0
    for step in range(1, tp_count):
        split, *whole = others[(step - 1) * each : step * each]
        rows = window(lax.rem(me - step + tp_count, tp_count) * 2 + h, split.shape[1])
        x = slab(split, whole, h)
        gate += dot(x, gate_ref[rows, :])
        up += dot(x, up_ref[rows, :])
    return gate, up


def early_kernel(tp_count, *refs):
    others, (gate_ref, up_ref, gate_acc, up_acc, gate_out, up_out) = refs[:-6], refs[-6:]
    gate, up = other_features(tp_count, 0, others, gate_ref, up_ref)
    gate_out[...] = gate_acc[...] + gate
    up_out[...] = up_acc[...] + up


def hidden_kernel(tp_count, count, places, *refs):
    others, refs = refs[:count], refs[count:]
    (gate_acc, up_acc, gate_ref, up_ref, down_ref, hidden_out), outs = refs[:6], refs[6:]
    me = lax.axis_index("tp")
    part = gate_ref.shape[0] // tp_count
    gate, up = other_features(tp_count, 1, others, gate_ref, up_ref)
    gate += gate_acc[...]
    up += up_acc[...]
    hidden = (gate / (1.0 + jnp.exp(-gate)) * up).astype(jnp.bfloat16)
    hidden_out[...] = hidden
    for step in range(1, tp_count):
        columns = window(lax.rem(me + step, tp_count), part)
        partial = dot(hidden, down_ref[:, columns]).astype(jnp.bfloat16)
        for place, out in zip(places, outs[(step - 1) * len(places) :]):
            size = out.shape[0] // len(place)
            for i, p in enumerate(place):
                out[pl.ds(i * size, size), :] = partial[p * size : (p + 1) * size]


def down_kernel(hidden_ref, down_ref, out_ref):
    columns = window(lax.axis_index("tp"), out_ref.shape[1])
    out_ref[...] = dot(hidden_ref[...], down_ref[:, columns])


def pack_kernel(place, arrived_count, mine_ref, *refs):
    arrived, outs = refs[:arrived_count], refs[arrived_count:]
    size = outs[0].shape[0]
    for i, (p, out) in enumerate(zip(place, outs)):
        total = mine_ref[pl.ds(p * size, size), :]
        for piece in arrived:
            total += piece[pl.ds(i * size, size), :].astype(jnp.float32)
        out[...] = total.astype(jnp.bfloat16)


def coefficient_kernel(ids_ref, scores_ref, out_ref):
    tok_rows = ids_ref.shape[1]
    me = lax.axis_index("ep")
    gains = jax.nn.sigmoid(scores_ref[...])
    weights = gains / jnp.sum(gains, 0, keepdims=True) * route_scale
    ids = ids_ref[...]
    diagonal = lax.broadcasted_iota(jnp.int32, (tok_rows, tok_rows), 0) == (
        lax.broadcasted_iota(jnp.int32, (tok_rows, tok_rows), 1)
    )
    for s in range(out_ref.shape[0] // tok_rows):
        row = jnp.sum(jnp.where(ids == (me ^ s), weights, 0.0), 0, keepdims=True)
        column = jnp.sum(jnp.where(diagonal, row, 0.0), 1, keepdims=True)
        out_ref[pl.ds(s * tok_rows, tok_rows), :] = jnp.broadcast_to(column, (tok_rows, LANES))


def combine_kernel(coefficient_ref, sum_ref, swapped_ref, *refs):
    pieces, (out_ref, counts_ref) = refs[:-2], refs[-2:]
    ep_count = len(pieces)
    tok_rows, part = out_ref.shape
    coefficients = [
        coefficient_ref[pl.ds(s * tok_rows, tok_rows), :] for s in range(ep_count)
    ]
    for lane in range(0, part, LANES):
        total = 0.0
        for coefficient, piece in zip(coefficients, pieces):
            total += coefficient * piece[:, lane : lane + LANES].astype(jnp.float32)
        out_ref[:, lane : lane + LANES] = total.astype(jnp.bfloat16)
    counts = sum_ref[...] + swapped_ref[...]
    for group in range(0, counts_ref.shape[0], tok_rows):
        size = min(tok_rows, counts_ref.shape[0] - group)
        start = group // tok_rows * LANES
        counts_ref[pl.ds(group, size), :] = counts[:size, start : start + ep_count]


def vmem_call(kernel, outs, args, flops):
    return pl.pallas_call(
        kernel,
        out_shape=[pltpu.VMEM(shape, dtype) for shape, dtype in outs],
        in_specs=[pl.BlockSpec(memory_space=pltpu.VMEM)] * len(args),
        out_specs=[pl.BlockSpec(memory_space=pltpu.VMEM)] * len(outs),
        compiler_params=pltpu.CompilerParams(vmem_limit_bytes=24 * MIB),
        cost_estimate=pl.CostEstimate(flops=flops, bytes_accessed=MIB, transcendentals=0),
    )(*args)


def per_device(tokens, expert_ids, replicas, scores, w_gate, w_up, w_down):
    rep_count = lax.axis_size("rep")
    ep_count = lax.axis_size("ep")
    tp_count = lax.axis_size("tp")
    tok_rows, part = tokens.shape
    ffe = w_gate.shape[2]
    rows = ep_count * tok_rows
    group, direct, out_groups = row_groups(ep_count)
    order = group + direct
    places = [[order.index(s) for s in group] for group in out_groups]
    bf16, f32, i32 = jnp.bfloat16, jnp.float32, jnp.int32
    gate_w, up_w, down_w = w_gate[0], w_up[0], w_down[0]

    ids, picks, gains = expert_ids.T, replicas.T, scores.T

    (ready,) = vmem_call(ready_kernel, [((8, LANES), f32)], (), 10**11)

    width = -(-rep_count // tok_rows) * LANES
    (message,) = vmem_call(
        functools.partial(intake_kernel, rep_count),
        [((tok_rows, part + width), bf16)],
        (tokens, ids, picks, ready),
        1000,
    )

    blocks = [message]
    blocks += [swap(message, "ep", ep_count, s) for s in range(1, ep_count)]
    steps = range(1, tp_count)
    shape = (len(group) * tok_rows, part // 2)
    halves = vmem_call(stack_kernel, [(shape, bf16)] * 2, tuple(blocks[s] for s in group), 1000)
    exchanged = []
    for held in halves:
        exchanged.append([shift(held, "tp", tp_count, d) for d in steps])
    across = []
    for s in direct:
        across.append([diagonal(tokens, ep_count, tp_count, s, d) for d in steps])
    others = [
        [ref for d in steps for ref in (exchanged[h][d - 1], *[a[d - 1] for a in across])]
        for h in range(2)
    ]
    (counts,) = vmem_call(sum_kernel, [((tok_rows, width), i32)], tuple(blocks), 1000)
    swapped = jnp.zeros_like(counts)
    for bit in range(rep_count.bit_length() - 1):
        counts = counts + swapped
        swapped = swap(counts, "rep", rep_count, rep_count >> (bit + 1))
    dot_flops = 2 * rows * part * ffe
    gate_acc, up_acc = vmem_call(
        own_kernel,
        [((rows, ffe), f32)] * 2,
        (*halves, *[blocks[s] for s in direct], gate_w, up_w, down_w),
        2 * dot_flops,
    )
    gate_acc, up_acc = vmem_call(
        functools.partial(early_kernel, tp_count),
        [((rows, ffe), f32)] * 2,
        (*others[0], gate_w, up_w, gate_acc, up_acc),
        dot_flops,
    )
    hidden, *partials = vmem_call(
        functools.partial(hidden_kernel, tp_count, len(others[1]), places),
        [((rows, ffe), bf16)]
        + [((len(p) * tok_rows, part), bf16) for p in places] * len(steps),
        (*others[1], gate_acc, up_acc, gate_w, up_w, down_w),
        3 * len(steps) * dot_flops,
    )
    arrived = []
    for number in range(len(places)):
        pieces = partials[number :: len(places)]
        arrived.append([shift(p, "tp", tp_count, s) for s, p in zip(steps, pieces)])
    (mine,) = vmem_call(down_kernel, [((rows, part), f32)], (hidden, down_w), dot_flops)

    back = [None] * ep_count
    for number, group in enumerate(out_groups):
        outgoing = vmem_call(
            functools.partial(pack_kernel, places[number], len(steps)),
            [((tok_rows, part), bf16)] * len(group),
            (mine, *arrived[number]),
            1000,
        )
        for s, piece in zip(group, outgoing):
            back[s] = swap(piece, "ep", ep_count, s) if s else piece
    (coefficients,) = vmem_call(coefficient_kernel, [((rows, LANES), f32)], (ids, gains), 1000)
    return pl.pallas_call(
        combine_kernel,
        out_shape=[
            jax.ShapeDtypeStruct((tok_rows, part), bf16),
            jax.ShapeDtypeStruct((rep_count, ep_count), i32),
        ],
        compiler_params=pltpu.CompilerParams(vmem_limit_bytes=8 * MIB),
        name="combine",
    )(coefficients, counts, swapped, *back)


def row_groups(ep_count):
    half = ep_count // 2
    far = list(range(ep_count - 1, half, -1))
    near = list(range(1, half))
    return [0, half] + near, far, [[half], far, near + [0]]


def solution(mesh):
    placed = (
        P(("rep", "ep"), "tp"),
        P(("rep", "ep"), None),
        P(("rep", "ep"), None),
        P(("rep", "ep"), None),
        P("ep", None, "tp"),
        P("ep", None, "tp"),
        P("ep", "tp", None),
    )

    return jax.shard_map(
        per_device,
        mesh=mesh,
        in_specs=placed,
        out_specs=(P(("rep", "ep"), "tp"), P()),
        check_vma=False,
    )
```

```python
import functools

import jax
import jax.numpy as jnp
from jax import lax
from jax.experimental import pallas as pl
from jax.experimental.pallas import tpu as pltpu
from jax.sharding import PartitionSpec as P

REPL = 4
LANES = 128
MIB = 1 << 20

route_scale = 2.5


def shift(array, axis, count, step):
    return lax.ppermute(array, axis, [(i, (i + step) % count) for i in range(count)])


def swap(array, axis, count, span):
    return lax.ppermute(array, axis, [(i, i ^ span) for i in range(count)])


def diagonal(array, ep_count, tp_count, span, step):
    pairs = [
        (e * tp_count + t, (e ^ span) * tp_count + (t + step) % tp_count)
        for e in range(ep_count)
        for t in range(tp_count)
    ]
    return lax.ppermute(array, ("ep", "tp"), pairs)


def window(index, size):
    return pl.ds(pl.multiple_of(index * size, size), size)


def dot(a, b):
    return jnp.dot(a, b, preferred_element_type=jnp.float32)


def ready_kernel(out_ref):
    out_ref[...] = jnp.zeros(out_ref.shape, out_ref.dtype)


def intake_kernel(rep_count, tokens_ref, ids_ref, picks_ref, ready_ref, out_ref):
    part = tokens_ref.shape[1]
    group = (lax.axis_index("rep") + picks_ref[...] * (rep_count // REPL)) & (rep_count - 1)
    ids = ids_ref[...]
    rows, lanes = out_ref.shape[0], out_ref.shape[1] - part
    cells = group * lanes + ids
    for wrap in range(rows, rep_count, rows):
        cells += jnp.where(group >= wrap, LANES - rows * lanes, 0)
    position = lax.broadcasted_iota(jnp.int32, (rows, lanes), 0) * lanes
    position = position + lax.broadcasted_iota(jnp.int32, (rows, lanes), 1)
    total = jnp.zeros((rows, lanes), jnp.float32)
    for k in range(cells.shape[0]):
        for t in range(cells.shape[1]):
            total += (position == cells[k : k + 1, t : t + 1]).astype(jnp.float32)
    out_ref[:, :part] = tokens_ref[...]
    out_ref[:, part:] = total.astype(out_ref.dtype)


def stack_kernel(*refs):
    pieces, outs = refs[:-2], refs[-2:]
    tok_rows, size = pieces[0].shape[0], outs[0].shape[1]
    for s, piece in enumerate(pieces):
        for h, out in enumerate(outs):
            out[pl.ds(s * tok_rows, tok_rows), :] = piece[:, h * size : (h + 1) * size]


def sum_kernel(*refs):
    pieces, out_ref = refs[:-1], refs[-1]
    part = pieces[0].shape[1] - out_ref.shape[1]
    out_ref[...] = sum(piece[:, part:].astype(jnp.float32) for piece in pieces).astype(jnp.int32)


def slab(split_ref, whole_refs, h):
    size = split_ref.shape[1]
    pieces = [split_ref[...]] + [ref[:, h * size : (h + 1) * size] for ref in whole_refs]
    return jnp.concatenate(pieces, 0)


def own_kernel(*refs):
    splits, pieces = refs[:2], refs[2:-5]
    gate_ref, up_ref, _, gate_acc, up_acc = refs[-5:]
    size = splits[0].shape[1]
    gate, up = 0.0, 0.0
    for h, split in enumerate(splits):
        rows = window(lax.axis_index("tp") * 2 + h, size)
        x = slab(split, pieces, h)
        gate += dot(x, gate_ref[rows, :])
        up += dot(x, up_ref[rows, :])
    gate_acc[...] = gate
    up_acc[...] = up


def other_features(tp_count, h, others, gate_ref, up_ref):
    me = lax.axis_index("tp")
    each = len(others) // (tp_count - 1)
    gate, up = 0.0, 0.0
    for step in range(1, tp_count):
        split, *whole = others[(step - 1) * each : step * each]
        rows = window(lax.rem(me - step + tp_count, tp_count) * 2 + h, split.shape[1])
        x = slab(split, whole, h)
        gate += dot(x, gate_ref[rows, :])
        up += dot(x, up_ref[rows, :])
    return gate, up


def early_kernel(tp_count, *refs):
    others, (gate_ref, up_ref, gate_acc, up_acc, gate_out, up_out) = refs[:-6], refs[-6:]
    gate, up = other_features(tp_count, 0, others, gate_ref, up_ref)
    gate_out[...] = gate_acc[...] + gate
    up_out[...] = up_acc[...] + up


def hidden_kernel(tp_count, count, places, *refs):
    others, refs = refs[:count], refs[count:]
    (gate_acc, up_acc, gate_ref, up_ref, down_ref, hidden_out), outs = refs[:6], refs[6:]
    me = lax.axis_index("tp")
    part = gate_ref.shape[0] // tp_count
    gate, up = other_features(tp_count, 1, others, gate_ref, up_ref)
    gate += gate_acc[...]
    up += up_acc[...]
    hidden = (gate / (1.0 + jnp.exp(-gate)) * up).astype(jnp.bfloat16)
    hidden_out[...] = hidden
    for step in range(1, tp_count):
        columns = window(lax.rem(me + step, tp_count), part)
        partial = dot(hidden, down_ref[:, columns]).astype(jnp.bfloat16)
        for place, out in zip(places, outs[(step - 1) * len(places) :]):
            size = out.shape[0] // len(place)
            for i, p in enumerate(place):
                out[pl.ds(i * size, size), :] = partial[p * size : (p + 1) * size]


def down_kernel(hidden_ref, down_ref, out_ref):
    columns = window(lax.axis_index("tp"), out_ref.shape[1])
    out_ref[...] = dot(hidden_ref[...], down_ref[:, columns])


def pack_kernel(place, arrived_count, mine_ref, *refs):
    arrived, outs = refs[:arrived_count], refs[arrived_count:]
    size = outs[0].shape[0]
    for i, (p, out) in enumerate(zip(place, outs)):
        total = mine_ref[pl.ds(p * size, size), :]
        for piece in arrived:
            total += piece[pl.ds(i * size, size), :].astype(jnp.float32)
        out[...] = total.astype(jnp.bfloat16)


def coefficient_kernel(ids_ref, scores_ref, out_ref):
    tok_rows = ids_ref.shape[1]
    me = lax.axis_index("ep")
    gains = jax.nn.sigmoid(scores_ref[...])
    weights = gains / jnp.sum(gains, 0, keepdims=True) * route_scale
    ids = ids_ref[...]
    diagonal = lax.broadcasted_iota(jnp.int32, (tok_rows, tok_rows), 0) == (
        lax.broadcasted_iota(jnp.int32, (tok_rows, tok_rows), 1)
    )
    for s in range(out_ref.shape[0] // tok_rows):
        row = jnp.sum(jnp.where(ids == (me ^ s), weights, 0.0), 0, keepdims=True)
        column = jnp.sum(jnp.where(diagonal, row, 0.0), 1, keepdims=True)
        out_ref[pl.ds(s * tok_rows, tok_rows), :] = jnp.broadcast_to(column, (tok_rows, LANES))


def table_kernel(ep_count, sum_ref, swapped_ref, counts_ref):
    counts = sum_ref[...] + swapped_ref[...]
    tok_rows = counts.shape[0]
    for group in range(0, counts_ref.shape[0], tok_rows):
        size = min(tok_rows, counts_ref.shape[0] - group)
        start = group // tok_rows * LANES
        counts_ref[pl.ds(group, size), :] = counts[:size, start : start + ep_count]


def weighted_kernel(blocks, has_start, coefficient_ref, *refs):
    start, pieces, out_ref = refs[:has_start], refs[has_start:-1], refs[-1]
    tok_rows, part = out_ref.shape
    coefficients = [coefficient_ref[pl.ds(s * tok_rows, tok_rows), :] for s in blocks]
    for lane in range(0, part, LANES):
        span = slice(lane, lane + LANES)
        total = start[0][:, span] if start else 0.0
        for coefficient, piece in zip(coefficients, pieces):
            total += coefficient * piece[:, span].astype(jnp.float32)
        out_ref[:, span] = total.astype(out_ref.dtype)


def vmem_call(kernel, outs, args, flops):
    return pl.pallas_call(
        kernel,
        out_shape=[pltpu.VMEM(shape, dtype) for shape, dtype in outs],
        in_specs=[pl.BlockSpec(memory_space=pltpu.VMEM)] * len(args),
        out_specs=[pl.BlockSpec(memory_space=pltpu.VMEM)] * len(outs),
        compiler_params=pltpu.CompilerParams(vmem_limit_bytes=24 * MIB),
        cost_estimate=pl.CostEstimate(flops=flops, bytes_accessed=MIB, transcendentals=0),
    )(*args)


def output_call(kernel, shape, dtype, args):
    return pl.pallas_call(
        kernel,
        out_shape=jax.ShapeDtypeStruct(shape, dtype),
        compiler_params=pltpu.CompilerParams(vmem_limit_bytes=8 * MIB),
    )(*args)


def per_device(tokens, expert_ids, replicas, scores, w_gate, w_up, w_down):
    rep_count = lax.axis_size("rep")
    ep_count = lax.axis_size("ep")
    tp_count = lax.axis_size("tp")
    tok_rows, part = tokens.shape
    ffe = w_gate.shape[2]
    rows = ep_count * tok_rows
    group, direct, out_groups = row_groups(ep_count)
    order = group + direct
    places = [[order.index(s) for s in group] for group in out_groups]
    bf16, f32, i32 = jnp.bfloat16, jnp.float32, jnp.int32
    gate_w, up_w, down_w = w_gate[0], w_up[0], w_down[0]

    ids, picks, gains = expert_ids.T, replicas.T, scores.T

    (ready,) = vmem_call(ready_kernel, [((8, LANES), f32)], (), 10**11)

    width = -(-rep_count // tok_rows) * LANES
    (message,) = vmem_call(
        functools.partial(intake_kernel, rep_count),
        [((tok_rows, part + width), bf16)],
        (tokens, ids, picks, ready),
        1000,
    )

    blocks = [message]
    blocks += [swap(message, "ep", ep_count, s) for s in range(1, ep_count)]
    steps = range(1, tp_count)
    shape = (len(group) * tok_rows, part // 2)
    halves = vmem_call(stack_kernel, [(shape, bf16)] * 2, tuple(blocks[s] for s in group), 1000)
    exchanged = []
    for held in halves:
        exchanged.append([shift(held, "tp", tp_count, d) for d in steps])
    across = []
    for s in direct:
        across.append([diagonal(tokens, ep_count, tp_count, s, d) for d in steps])
    others = [
        [ref for d in steps for ref in (exchanged[h][d - 1], *[a[d - 1] for a in across])]
        for h in range(2)
    ]
    (counts,) = vmem_call(sum_kernel, [((tok_rows, width), i32)], tuple(blocks), 1000)
    swapped = jnp.zeros_like(counts)
    for bit in range(rep_count.bit_length() - 1):
        counts = counts + swapped
        swapped = swap(counts, "rep", rep_count, rep_count >> (bit + 1))
    dot_flops = 2 * rows * part * ffe
    gate_acc, up_acc = vmem_call(
        own_kernel,
        [((rows, ffe), f32)] * 2,
        (*halves, *[blocks[s] for s in direct], gate_w, up_w, down_w),
        2 * dot_flops,
    )
    gate_acc, up_acc = vmem_call(
        functools.partial(early_kernel, tp_count),
        [((rows, ffe), f32)] * 2,
        (*others[0], gate_w, up_w, gate_acc, up_acc),
        dot_flops,
    )
    hidden, *partials = vmem_call(
        functools.partial(hidden_kernel, tp_count, len(others[1]), places),
        [((rows, ffe), bf16)]
        + [((len(p) * tok_rows, part), bf16) for p in places] * len(steps),
        (*others[1], gate_acc, up_acc, gate_w, up_w, down_w),
        3 * len(steps) * dot_flops,
    )
    arrived = []
    for number in range(len(places)):
        pieces = partials[number :: len(places)]
        arrived.append([shift(p, "tp", tp_count, s) for s, p in zip(steps, pieces)])
    (mine,) = vmem_call(down_kernel, [((rows, part), f32)], (hidden, down_w), dot_flops)

    back = [None] * ep_count
    for number, group in enumerate(out_groups):
        outgoing = vmem_call(
            functools.partial(pack_kernel, places[number], len(steps)),
            [((tok_rows, part), bf16)] * len(group),
            (mine, *arrived[number]),
            1000,
        )
        for s, piece in zip(group, outgoing):
            back[s] = swap(piece, "ep", ep_count, s) if s else piece
    (coefficients,) = vmem_call(coefficient_kernel, [((rows, LANES), f32)], (ids, gains), 1000)
    load_counts = output_call(
        functools.partial(table_kernel, ep_count), (rep_count, ep_count), i32, (counts, swapped)
    )
    first = [0, *out_groups[0]]
    (begun,) = vmem_call(
        functools.partial(weighted_kernel, first, 0),
        [((tok_rows, part), f32)],
        (coefficients, *[back[s] for s in first]),
        1000,
    )
    later = [s for s in range(ep_count) if s not in first]
    moe_out = output_call(
        functools.partial(weighted_kernel, later, 1),
        (tok_rows, part),
        bf16,
        (coefficients, begun, *[back[s] for s in later]),
    )
    return moe_out, load_counts


def row_groups(ep_count):
    half = ep_count // 2
    far = list(range(ep_count - 1, half, -1))
    near = list(range(1, half))
    return [0, half] + near, far, [[half], far, near + [0]]


def solution(mesh):
    placed = (
        P(("rep", "ep"), "tp"),
        P(("rep", "ep"), None),
        P(("rep", "ep"), None),
        P(("rep", "ep"), None),
        P("ep", None, "tp"),
        P("ep", None, "tp"),
        P("ep", "tp", None),
    )

    return jax.shard_map(
        per_device,
        mesh=mesh,
        in_specs=placed,
        out_specs=(P(("rep", "ep"), "tp"), P()),
        check_vma=False,
    )
```

```python
import functools

import jax
import jax.numpy as jnp
from jax import lax
from jax.experimental import pallas as pl
from jax.experimental.pallas import tpu as pltpu
from jax.sharding import PartitionSpec as P

REPL = 4
LANES = 128
MIB = 1 << 20

route_scale = 2.5


def shift(array, axis, count, step):
    return lax.ppermute(array, axis, [(i, (i + step) % count) for i in range(count)])


def swap(array, axis, count, span):
    return lax.ppermute(array, axis, [(i, i ^ span) for i in range(count)])


def diagonal(array, ep_count, tp_count, span, step):
    pairs = [
        (e * tp_count + t, (e ^ span) * tp_count + (t + step) % tp_count)
        for e in range(ep_count)
        for t in range(tp_count)
    ]
    return lax.ppermute(array, ("ep", "tp"), pairs)


def window(index, size):
    return pl.ds(pl.multiple_of(index * size, size), size)


def dot(a, b):
    return jnp.dot(a, b, preferred_element_type=jnp.float32)


def ready_kernel(out_ref):
    out_ref[...] = jnp.zeros(out_ref.shape, out_ref.dtype)


def intake_kernel(rep_count, tokens_ref, ids_ref, picks_ref, ready_ref, out_ref):
    part = tokens_ref.shape[1]
    group = (lax.axis_index("rep") + picks_ref[...] * (rep_count // REPL)) & (rep_count - 1)
    ids = ids_ref[...]
    rows, lanes = out_ref.shape[0], out_ref.shape[1] - part
    cells = group * lanes + ids
    for wrap in range(rows, rep_count, rows):
        cells += jnp.where(group >= wrap, LANES - rows * lanes, 0)
    position = lax.broadcasted_iota(jnp.int32, (rows, lanes), 0) * lanes
    position = position + lax.broadcasted_iota(jnp.int32, (rows, lanes), 1)
    total = jnp.zeros((rows, lanes), jnp.float32)
    for k in range(cells.shape[0]):
        for t in range(cells.shape[1]):
            total += (position == cells[k : k + 1, t : t + 1]).astype(jnp.float32)
    out_ref[:, :part] = tokens_ref[...]
    out_ref[:, part:] = total.astype(out_ref.dtype)


def stack_kernel(*refs):
    pieces, outs = refs[:-2], refs[-2:]
    tok_rows, size = pieces[0].shape[0], outs[0].shape[1]
    for s, piece in enumerate(pieces):
        for h, out in enumerate(outs):
            out[pl.ds(s * tok_rows, tok_rows), :] = piece[:, h * size : (h + 1) * size]


def sum_kernel(*refs):
    pieces, out_ref = refs[:-1], refs[-1]
    part = pieces[0].shape[1] - out_ref.shape[1]
    out_ref[...] = sum(piece[:, part:].astype(jnp.float32) for piece in pieces).astype(jnp.int32)


def slab(split_ref, whole_refs, h):
    size = split_ref.shape[1]
    pieces = [split_ref[...]] + [ref[:, h * size : (h + 1) * size] for ref in whole_refs]
    return jnp.concatenate(pieces, 0)


def own_kernel(*refs):
    splits, pieces = refs[:2], refs[2:-5]
    gate_ref, up_ref, _, gate_acc, up_acc = refs[-5:]
    size = splits[0].shape[1]
    gate, up = 0.0, 0.0
    for h, split in enumerate(splits):
        rows = window(lax.axis_index("tp") * 2 + h, size)
        x = slab(split, pieces, h)
        gate += dot(x, gate_ref[rows, :])
        up += dot(x, up_ref[rows, :])
    gate_acc[...] = gate
    up_acc[...] = up


def other_features(tp_count, h, others, gate_ref, up_ref):
    me = lax.axis_index("tp")
    each = len(others) // (tp_count - 1)
    gate, up = 0.0, 0.0
    for step in range(1, tp_count):
        split, *whole = others[(step - 1) * each : step * each]
        rows = window(lax.rem(me - step + tp_count, tp_count) * 2 + h, split.shape[1])
        x = slab(split, whole, h)
        gate += dot(x, gate_ref[rows, :])
        up += dot(x, up_ref[rows, :])
    return gate, up


def early_kernel(tp_count, *refs):
    others, (gate_ref, up_ref, gate_acc, up_acc, gate_out, up_out) = refs[:-6], refs[-6:]
    gate, up = other_features(tp_count, 0, others, gate_ref, up_ref)
    gate_out[...] = gate_acc[...] + gate
    up_out[...] = up_acc[...] + up


def hidden_kernel(tp_count, count, places, *refs):
    others, refs = refs[:count], refs[count:]
    (gate_acc, up_acc, gate_ref, up_ref, down_ref, hidden_out), outs = refs[:6], refs[6:]
    me = lax.axis_index("tp")
    part = gate_ref.shape[0] // tp_count
    gate, up = other_features(tp_count, 1, others, gate_ref, up_ref)
    gate += gate_acc[...]
    up += up_acc[...]
    hidden = (gate / (1.0 + jnp.exp(-gate)) * up).astype(jnp.bfloat16)
    hidden_out[...] = hidden
    for step in range(1, tp_count):
        columns = window(lax.rem(me + step, tp_count), part)
        partial = dot(hidden, down_ref[:, columns]).astype(jnp.bfloat16)
        for place, out in zip(places, outs[(step - 1) * len(places) :]):
            size = out.shape[0] // len(place)
            for i, p in enumerate(place):
                out[pl.ds(i * size, size), :] = partial[p * size : (p + 1) * size]


def down_kernel(hidden_ref, down_ref, out_ref):
    columns = window(lax.axis_index("tp"), out_ref.shape[1])
    out_ref[...] = dot(hidden_ref[...], down_ref[:, columns])


def pack_kernel(place, arrived_count, mine_ref, counts_ref, swapped_ref, *refs):
    arrived, outs = refs[:arrived_count], refs[arrived_count:]
    size, part = outs[0].shape[0], mine_ref.shape[1]
    for i, (p, out) in enumerate(zip(place, outs)):
        total = mine_ref[pl.ds(p * size, size), :]
        for piece in arrived:
            total += piece[pl.ds(i * size, size), :].astype(jnp.float32)
        out[:, :part] = total.astype(jnp.bfloat16)
        if out.shape[1] > part:
            carried = counts_ref[...] + swapped_ref[...]
            out[:, part:] = carried.astype(jnp.float32).astype(jnp.bfloat16)


def coefficient_kernel(ids_ref, scores_ref, out_ref):
    tok_rows = ids_ref.shape[1]
    me = lax.axis_index("ep")
    gains = jax.nn.sigmoid(scores_ref[...])
    weights = gains / jnp.sum(gains, 0, keepdims=True) * route_scale
    ids = ids_ref[...]
    diagonal = lax.broadcasted_iota(jnp.int32, (tok_rows, tok_rows), 0) == (
        lax.broadcasted_iota(jnp.int32, (tok_rows, tok_rows), 1)
    )
    for s in range(out_ref.shape[0] // tok_rows):
        row = jnp.sum(jnp.where(ids == (me ^ s), weights, 0.0), 0, keepdims=True)
        column = jnp.sum(jnp.where(diagonal, row, 0.0), 1, keepdims=True)
        out_ref[pl.ds(s * tok_rows, tok_rows), :] = jnp.broadcast_to(column, (tok_rows, LANES))


def weighted_kernel(blocks, has_start, coefficient_ref, *refs):
    start, pieces, out_ref = refs[:has_start], refs[has_start:-1], refs[-1]
    tok_rows, part = out_ref.shape
    coefficients = [coefficient_ref[pl.ds(s * tok_rows, tok_rows), :] for s in blocks]
    for lane in range(0, part, LANES):
        span = slice(lane, lane + LANES)
        total = start[0][:, span] if start else 0.0
        for coefficient, piece in zip(coefficients, pieces):
            total += coefficient * piece[:, span].astype(jnp.float32)
        out_ref[:, span] = total.astype(out_ref.dtype)


def finish_kernel(blocks, coefficient_ref, sum_ref, swapped_ref, begun_ref, *refs):
    pieces, (out_ref, counts_ref) = refs[:-2], refs[-2:]
    weighted_kernel(blocks, 1, coefficient_ref, begun_ref, *pieces, out_ref)
    tok_rows, part = out_ref.shape
    counts = sum_ref[...] + swapped_ref[...]
    counts += pieces[-1][:, part:].astype(jnp.float32).astype(jnp.int32)
    for group in range(0, counts_ref.shape[0], tok_rows):
        size = min(tok_rows, counts_ref.shape[0] - group)
        start = group // tok_rows * LANES
        columns = counts_ref.shape[1]
        counts_ref[pl.ds(group, size), :] = counts[:size, start : start + columns]


def vmem_call(kernel, outs, args, flops):
    return pl.pallas_call(
        kernel,
        out_shape=[pltpu.VMEM(shape, dtype) for shape, dtype in outs],
        in_specs=[pl.BlockSpec(memory_space=pltpu.VMEM)] * len(args),
        out_specs=[pl.BlockSpec(memory_space=pltpu.VMEM)] * len(outs),
        compiler_params=pltpu.CompilerParams(vmem_limit_bytes=24 * MIB),
        cost_estimate=pl.CostEstimate(flops=flops, bytes_accessed=MIB, transcendentals=0),
    )(*args)


def per_device(tokens, expert_ids, replicas, scores, w_gate, w_up, w_down):
    rep_count = lax.axis_size("rep")
    ep_count = lax.axis_size("ep")
    tp_count = lax.axis_size("tp")
    tok_rows, part = tokens.shape
    ffe = w_gate.shape[2]
    rows = ep_count * tok_rows
    group, direct, out_groups = row_groups(ep_count)
    order = group + direct
    places = [[order.index(s) for s in group] for group in out_groups]
    bf16, f32, i32 = jnp.bfloat16, jnp.float32, jnp.int32
    gate_w, up_w, down_w = w_gate[0], w_up[0], w_down[0]

    ids, picks, gains = expert_ids.T, replicas.T, scores.T

    (ready,) = vmem_call(ready_kernel, [((8, LANES), f32)], (), 10**11)

    width = -(-rep_count // tok_rows) * LANES
    (message,) = vmem_call(
        functools.partial(intake_kernel, rep_count),
        [((tok_rows, part + width), bf16)],
        (tokens, ids, picks, ready),
        1000,
    )

    half = ep_count // 2
    blocks = [message]
    for s in range(1, ep_count):
        blocks.append(swap(message if s < half else tokens, "ep", ep_count, s))
    steps = range(1, tp_count)
    shape = (len(group) * tok_rows, part // 2)
    halves = vmem_call(stack_kernel, [(shape, bf16)] * 2, tuple(blocks[s] for s in group), 1000)
    exchanged = []
    for held in halves:
        exchanged.append([shift(held, "tp", tp_count, d) for d in steps])
    across = []
    for s in direct:
        across.append([diagonal(tokens, ep_count, tp_count, s, d) for d in steps])
    others = [
        [ref for d in steps for ref in (exchanged[h][d - 1], *[a[d - 1] for a in across])]
        for h in range(2)
    ]
    (counts,) = vmem_call(sum_kernel, [((tok_rows, width), i32)], tuple(blocks[:half]), 1000)
    swapped = jnp.zeros_like(counts)
    for bit in range(rep_count.bit_length() - 1):
        counts = counts + swapped
        swapped = swap(counts, "rep", rep_count, rep_count >> (bit + 1))
    dot_flops = 2 * rows * part * ffe
    gate_acc, up_acc = vmem_call(
        own_kernel,
        [((rows, ffe), f32)] * 2,
        (*halves, *[blocks[s] for s in direct], gate_w, up_w, down_w),
        2 * dot_flops,
    )
    gate_acc, up_acc = vmem_call(
        functools.partial(early_kernel, tp_count),
        [((rows, ffe), f32)] * 2,
        (*others[0], gate_w, up_w, gate_acc, up_acc),
        dot_flops,
    )
    hidden, *partials = vmem_call(
        functools.partial(hidden_kernel, tp_count, len(others[1]), places),
        [((rows, ffe), bf16)]
        + [((len(p) * tok_rows, part), bf16) for p in places] * len(steps),
        (*others[1], gate_acc, up_acc, gate_w, up_w, down_w),
        3 * len(steps) * dot_flops,
    )
    arrived = []
    for number in range(len(places)):
        pieces = partials[number :: len(places)]
        arrived.append([shift(p, "tp", tp_count, s) for s, p in zip(steps, pieces)])
    (mine,) = vmem_call(down_kernel, [((rows, part), f32)], (hidden, down_w), dot_flops)

    back = [None] * ep_count
    for number, group in enumerate(out_groups):
        outgoing = vmem_call(
            functools.partial(pack_kernel, places[number], len(steps)),
            [((tok_rows, part + width * (s == ep_count - 1)), bf16) for s in group],
            (mine, counts, swapped, *arrived[number]),
            1000,
        )
        for s, piece in zip(group, outgoing):
            back[s] = swap(piece, "ep", ep_count, s) if s else piece
    (coefficients,) = vmem_call(coefficient_kernel, [((rows, LANES), f32)], (ids, gains), 1000)
    first = [0, *out_groups[0]]
    (begun,) = vmem_call(
        functools.partial(weighted_kernel, first, 0),
        [((tok_rows, part), f32)],
        (coefficients, *[back[s] for s in first]),
        1000,
    )
    later = [s for s in range(ep_count) if s not in first]
    return pl.pallas_call(
        functools.partial(finish_kernel, later),
        out_shape=[
            jax.ShapeDtypeStruct((tok_rows, part), bf16),
            jax.ShapeDtypeStruct((rep_count, ep_count), i32),
        ],
        compiler_params=pltpu.CompilerParams(vmem_limit_bytes=8 * MIB),
        name="finish",
    )(coefficients, counts, swapped, begun, *[back[s] for s in later])


def row_groups(ep_count):
    half = ep_count // 2
    far = list(range(ep_count - 1, half, -1))
    near = list(range(1, half))
    return [0, half] + near, far, [[half], far, near + [0]]


def solution(mesh):
    placed = (
        P(("rep", "ep"), "tp"),
        P(("rep", "ep"), None),
        P(("rep", "ep"), None),
        P(("rep", "ep"), None),
        P("ep", None, "tp"),
        P("ep", None, "tp"),
        P("ep", "tp", None),
    )

    return jax.shard_map(
        per_device,
        mesh=mesh,
        in_specs=placed,
        out_specs=(P(("rep", "ep"), "tp"), P()),
        check_vma=False,
    )
```
